8 devices in a mesh: rep: 1 (over z), dp: 8 (over x, y, core).
Axes of the slice: x: 2, y: 2, z: 1, core: 2. Of those that a mesh axis runs over, the one named last changes fastest.
Arguments:
- x: bfloat16 [8, 2048, 1024], P(('rep', 'dp'))
- dy: bfloat16 [8, 2048, 1024], P(('rep', 'dp'))
- w_gate: bfloat16 [2, 1024, 2816], P(None, 'dp')
- w_up: bfloat16 [2, 1024, 2816], P(None, 'dp')
- w_down: bfloat16 [2, 2816, 1024], P(None, 'dp')
Outputs:
- output 1: bfloat16 [8, 2048, 1024], P(('rep', 'dp'))
- output 2: bfloat16 [2, 1024, 2816], P('rep', 'dp')
- output 3: bfloat16 [2, 1024, 2816], P('rep', 'dp')
- output 4: bfloat16 [2, 2816, 1024], P('rep', 'dp')
All inputs are finite; a program needn't handle non-finite values.
Results may differ from the reference program's by a relative error of at most 0.018.
Values are sent between devices in bfloat16 or wider.
A program may use at most 2 GiB of HBM per device.

```python
import jax
import jax.numpy as jnp
from jax import lax

SEQUENCES = 8
TOKENS = 2048
D = 1024
FF = 2816
LAYERS = 2
NAMES = ("w_gate", "w_up", "w_down")
SHAPES = {"w_gate": (LAYERS, D, FF), "w_up": (LAYERS, D, FF), "w_down": (LAYERS, FF, D)}


def bump(key, n, height):
    away = (jnp.arange(n, dtype=jnp.int32) - jax.random.randint(key, (), 0, n, jnp.int32)) % n
    return jnp.where(away < n // 8, height, 1.0)


def together(key, own, strength):
    shared = jax.random.normal(key, own.shape[1:], jnp.float32)
    return (own + strength * shared) * lax.rsqrt(1 + strength * strength)


def setup_inputs(seed: int = 0, part: int = 0) -> dict:
    kx, kdy, ka, kb, kz, kf, kh, kl, *kw = jax.random.split(jax.random.key(seed), 8 + len(NAMES))
    kx, kdy, ka, kb = (jax.random.fold_in(k, part) for k in (kx, kdy, ka, kb))
    shape = (SEQUENCES, TOKENS, D)
    much_x, much_dy = jax.random.uniform(kz, (2,), jnp.float32, 0.0, 1.0)
    layers = 2.0 ** jax.random.uniform(kl, (LAYERS, 1, 1), jnp.float32, -1.0, 1.0)
    x = together(ka, jax.random.normal(kx, shape, jnp.float32), much_x) * bump(kf, D, 4.0)
    dy = together(kb, jax.random.normal(kdy, shape, jnp.float32), much_dy)
    drawn = {"x": x.astype(jnp.bfloat16), "dy": (dy * (SEQUENCES * TOKENS) ** -0.5).astype(jnp.bfloat16)}
    for key, name in zip(kw, NAMES, strict=True):
        w = jax.random.normal(key, SHAPES[name], jnp.float32) * SHAPES[name][1] ** -0.5
        drawn[name] = (w * {"w_gate": 1.0, "w_up": bump(kh, FF, 4.0), "w_down": layers}[name]).astype(jnp.bfloat16)
    return drawn


def matmul(a, w):
    return jnp.dot(a, w, preferred_element_type=jnp.float32).astype(jnp.bfloat16)


def normed(h):
    wide = h.astype(jnp.float32)
    scale = lax.rsqrt(jnp.mean(wide**2, -1, keepdims=True) + 1e-6)
    return (wide * scale).astype(jnp.bfloat16)


def layer(h, w):
    a = normed(h)
    gate = jnp.dot(a, w["w_gate"], preferred_element_type=jnp.float32)
    up = jnp.dot(a, w["w_up"], preferred_element_type=jnp.float32)
    return h + matmul((jax.nn.silu(gate) * up).astype(jnp.bfloat16), w["w_down"])


def stack(weights, h):
    return lax.scan(lambda h, w: (layer(h, w), None), h, weights)[0]


def reference(x, dy, w_gate, w_up, w_down):
    weights = dict(zip(NAMES, (w_gate, w_up, w_down), strict=True))

    def take(so_far, sequence):
        h, by_y = sequence
        _, back = jax.vjp(stack, weights, h)
        by_weights, by_h = back(by_y)
        return jax.tree.map(lambda total, term: total + term.astype(jnp.float32), so_far, by_weights), by_h

    none_yet = {name: jnp.zeros(w.shape, jnp.float32) for name, w in weights.items()}
    by_weights, by_x = lax.scan(take, none_yet, (x, dy))
    return (by_x, *(by_weights[name].astype(jnp.bfloat16) for name in NAMES))
```

```python
import jax
import jax.numpy as jnp
from jax import lax
from jax.experimental import pallas as pl
from jax.experimental.pallas import tpu as pltpu
from jax.sharding import PartitionSpec as P

BF, F32 = jnp.bfloat16, jnp.float32
T, D, FF = 2048, 1024, 2816
H = FF // 2
GROWS, DROWS = D // 8, FF // 8
UNITS = ((0, 0), (0, 1), (0, 2), (1, 2), (1, 0), (1, 1))
NT = (((1,), (1,)), ((), ()))
TN = (((0,), (0,)), ((), ()))
VMEM = pltpu.VMEM
ANY = pl.ANY
MIB = 1 << 20


def rows_of(u):
    return DROWS if UNITS[u][1] == 2 else GROWS


def full_shape(u):
    return (FF, D) if UNITS[u][1] == 2 else (D, FF)


def sigmoid(z):
    return 0.5 * jnp.tanh(0.5 * z) + 0.5


def dot(a, b):
    return jnp.dot(a, b, preferred_element_type=F32)


def dotg(a, b, dims):
    return lax.dot_general(a, b, dims, preferred_element_type=F32)


def places():
    me = lax.axis_index("dp")
    ix, iy, ic = me // 4, (me // 2) % 2, me % 2
    flip = lambda a, b, c: (ix + a - 2 * a * ix) * 4 + (iy + b - 2 * b * iy) * 2 + (ic + c - 2 * c * ic)
    return me, flip


def barrier(peers):
    sem = pltpu.get_barrier_semaphore()
    for p in peers:
        pl.semaphore_signal(sem, inc=1, device_id={"dp": p}, device_id_type=pl.DeviceIdType.MESH)
    pl.semaphore_wait(sem, len(peers))


def remote(src, dst, send, recv, to):
    return pltpu.make_async_remote_copy(src_ref=src, dst_ref=dst, send_sem=send, recv_sem=recv, device_id={"dp": to}, device_id_type=pl.DeviceIdType.MESH)


def block(rows, cols, index):
    return pl.BlockSpec((rows, cols), index)


def forward_kernel(x, dy, wg, wu, wd, *refs):
    full, refs = refs[:6], refs[6:]
    a0, a0t, h1, a1, a1t, act0, gu0, act1, dgu1, dact1, mixed, resident, down, send, recv, local, extra, mix = refs
    shards = [wd.at[n] if part == 2 else mixed.at[2 * n + part] for n, part in UNITS]
    me, flip = places()
    nx, ny, peer, nxy = flip(1, 0, 0), flip(0, 1, 0), flip(0, 0, 1), flip(1, 1, 0)

    def part(u, b, half=None):
        r = rows_of(u)
        if half is None:
            return full[u].at[pl.ds(b * r, r), :]
        return full[u].at[pl.ds(b * r + half * (r // 2), r // 2), :]

    def copy(u, k):
        own = shards[u]
        src, dst, to = (
            (own, part(u, me), nx),
            (own, part(u, me), ny),
            (own, part(u, me), peer),
            (part(u, nx, 0), part(u, nx, 0), ny),
            (part(u, ny, 1), part(u, ny, 1), nx),
            (part(u, nx), part(u, nx), peer),
            (part(u, ny), part(u, ny), peer),
            (part(u, nxy, 0), part(u, nxy, 0), peer),
            (part(u, nxy, 1), part(u, nxy, 1), peer),
        )[k]
        return remote(src, dst, send.at[u, k], recv.at[u, k], to)

    def own_copy(u):
        return pltpu.make_async_copy(shards[u], part(u, me), local.at[u])

    def start_own(u):
        for k in (0, 1, 2):
            copy(u, k).start()
        own_copy(u).start()

    def forward_one(u):
        copy(u, 0).wait_recv()
        copy(u, 3).start()
        copy(u, 5).start()
        copy(u, 1).wait_recv()
        copy(u, 4).start()
        copy(u, 6).start()

    def forward_two(u):
        copy(u, 3).wait_recv()
        copy(u, 7).start()
        copy(u, 4).wait_recv()
        copy(u, 8).start()

    def arrived(u):
        own_copy(u).wait()
        for k in (2, 5, 6, 7, 8):
            copy(u, k).wait_recv()

    def load(src, dst, n):
        return pltpu.make_async_copy(src, dst, extra.at[n])

    def norm_into(wide, a_ref, at_ref):
        scale = lax.rsqrt(jnp.mean(wide * wide, -1, keepdims=True) + 1e-6)
        a = wide * scale
        a_ref[...] = a.astype(BF)
        at_ref[...] = a.astype(BF).T

    def mix_start(u):
        n, part = UNITS[u]
        for j in range(11):
            cols = pl.ds(128 * (11 * part + j), 128)
            pltpu.make_async_copy(wg.at[n, :, cols], shards[u].at[:, pl.ds(256 * j, 128)], mix.at[u]).start()
            pltpu.make_async_copy(wu.at[n, :, cols], shards[u].at[:, pl.ds(256 * j + 128, 128)], mix.at[u]).start()

    def mix_wait(u):
        pltpu.make_async_copy(shards[u], shards[u], mix.at[u]).wait()

    for u in (0, 1, 4, 5):
        mix_start(u)
    barrier((nx, ny, peer))
    mix_wait(0)
    start_own(0)
    mix_wait(1)
    start_own(1)
    mix_wait(4)
    mix_wait(5)

    def norm_body(x_ref, a_ref, at_ref):
        norm_into(x_ref[...].astype(F32), a_ref, at_ref)

    pltpu.emit_pipeline(
        norm_body,
        grid=(T // 256,),
        in_specs=[block(256, D, lambda i: (i, 0))],
        out_specs=[block(256, D, lambda i: (i, 0)), block(D, 256, lambda i: (0, i))],
    )(x, a0, a0t)
    load(a0, resident, 0).start()

    forward_one(0)
    start_own(2)
    forward_two(0)
    forward_one(1)
    start_own(3)
    arrived(0)
    load(a0, resident, 0).wait()

    def gu0_body(w_ref, gu_ref, act_ref):
        for m in range(0, T, 512):
            s = dot(resident[m : m + 512, :], w_ref[...])
            gu_ref[m : m + 512, :] = s
            g, up = s[:, :128], s[:, 128:]
            act_ref[m : m + 512, :] = (g * sigmoid(g) * up).astype(BF)

    def gu0_op(half):
        pltpu.emit_pipeline(
            gu0_body,
            grid=(11,),
            in_specs=[block(D, 256, lambda j: (0, j))],
            out_specs=[block(T, 256, lambda j: (0, j + 11 * half)), block(T, 128, lambda j: (0, j + 11 * half))],
        )(full[half], gu0, act0)

    gu0_op(0)
    forward_two(1)
    forward_one(2)
    start_own(4)
    arrived(1)
    gu0_op(1)
    forward_two(2)
    forward_one(3)
    start_own(5)
    arrived(2)
    load(full[2], down, 1).start()
    load(dy, resident, 0).start()
    load(full[2], down, 1).wait()

    def down_body(act_ref, x_ref, h_ref, a_ref, at_ref):
        h = x_ref[...] + dot(act_ref[...], down[...]).astype(BF)
        h_ref[...] = h
        norm_into(h.astype(F32), a_ref, at_ref)

    tile = lambda i: (i, 0)
    pltpu.emit_pipeline(
        down_body,
        grid=(T // 512,),
        in_specs=[block(512, FF, tile), block(512, D, tile)],
        out_specs=[block(512, D, tile), block(512, D, tile), block(D, 512, lambda i: (0, i))],
    )(act0, x, h1, a1, a1t)
    load(dy, resident, 0).wait()
    forward_two(3)
    forward_one(4)
    arrived(3)

    def dact_body(w_ref, out_ref):
        for m in range(0, T, 512):
            out_ref[m : m + 512, :] = dotg(resident[m : m + 512, :], w_ref[...], NT).astype(BF)

    pltpu.emit_pipeline(
        dact_body,
        grid=(11,),
        in_specs=[block(256, D, lambda j: (j, 0))],
        out_specs=[block(T, 256, lambda j: (0, j))],
    )(full[3], dact1)
    load(a1, resident, 0).start()
    forward_two(4)
    forward_one(5)
    arrived(4)
    load(a1, resident, 0).wait()

    def gu1_body(w_ref, dact_ref, act_ref, dgu_ref):
        for m in range(0, T, 512):
            s = dot(resident[m : m + 512, :], w_ref[...])
            g, up = s[:, :128], s[:, 128:]
            d = dact_ref[m : m + 512, :].astype(F32)
            sg = sigmoid(g)
            silu = g * sg
            act_ref[m : m + 512, :] = (silu * up).astype(BF)
            dgu_ref[m : m + 512, :128] = (d * up * (sg + silu * (1.0 - sg))).astype(BF)
            dgu_ref[m : m + 512, 128:] = (d * silu).astype(BF)

    def gu1_op(half):
        col = lambda j: (0, j + 11 * half)
        pltpu.emit_pipeline(
            gu1_body,
            grid=(11,),
            in_specs=[block(D, 256, lambda j: (0, j)), block(T, 128, col)],
            out_specs=[block(T, 128, col), block(T, 256, col)],
        )(full[4 + half], dact1, act1, dgu1)

    gu1_op(0)
    forward_two(5)
    arrived(5)
    gu1_op(1)
    for u in range(6):
        for k in range(9):
            copy(u, k).wait_send()


def forward(x, dy, wg, wu, wd):
    vm, any_ = pl.BlockSpec(memory_space=VMEM), pl.BlockSpec(memory_space=ANY)
    s = jax.ShapeDtypeStruct
    outs = [s(full_shape(u), BF) for u in range(6)]
    outs += [s((T, D), BF), s((D, T), BF), s((T, D), BF), s((T, D), BF), s((D, T), BF)]
    outs += [s((T, FF), BF), s((T, 2 * FF), F32), s((T, FF), BF), s((T, 2 * FF), BF), s((T, FF), BF)]
    return pl.pallas_call(
        forward_kernel,
        out_shape=outs,
        in_specs=[any_, any_, any_, any_, vm],
        out_specs=[any_] * len(outs),
        scratch_shapes=[
            VMEM((4, GROWS, FF), BF),
            VMEM((T, D), BF),
            VMEM((FF, D), BF),
            pltpu.SemaphoreType.DMA((6, 9)),
            pltpu.SemaphoreType.DMA((6, 9)),
            pltpu.SemaphoreType.DMA((6,)),
            pltpu.SemaphoreType.DMA((2,)),
            pltpu.SemaphoreType.DMA((6,)),
        ],
        compiler_params=pltpu.CompilerParams(collective_id=0, has_side_effects=True, vmem_limit_bytes=60 * MIB),
        name="forward_gather",
    )(x, dy, wg, wu, wd)


def backward_kernel(x, h1, dy, a0t, a1t, act0, act1, gu0, dgu1, w00, w01, w02, w10, w11, *refs):
    (by_g, by_u, by_d, dx, dh1, dgu0), term, from_peer, refs = refs[:6], refs[6:12], refs[12:18], refs[18:]
    (weights, resident, resident_t, r1x, r1y, r2x, r2y, d1x, d1y, d2x, d2y, gsend, dsend, gload, dload, send, recv, lsem, extra, osem) = refs
    me, flip = places()
    nx, ny, peer, nxy = flip(1, 0, 0), flip(0, 1, 0), flip(0, 0, 1), flip(1, 1, 0)
    where = (me, nx, ny, nxy)

    def kind(u):
        return UNITS[u][1] == 2

    def slot(u):
        return {0: 0, 1: 1, 2: 0, 3: 1, 4: 2, 5: 3}[u]

    def landing(u):
        s = slot(u)
        return tuple(t.at[s] for t in ((d1x, d1y, d2x, d2y) if kind(u) else (r1x, r1y, r2x, r2y)))

    def sending(u):
        return dsend if kind(u) else gsend

    def loading(u):
        return dload if kind(u) else gload

    def peer_block(b):
        return b + 1 - 2 * (b % 2)

    def copy(u, k):
        r = rows_of(u)
        if k < 4:
            b = where[k]
            return remote(term[u].at[pl.ds(peer_block(b) * r, r), :], from_peer[u].at[pl.ds((b // 2) * r, r), :], send.at[u, k], recv.at[u, k], peer)
        s, (l1x, l1y, l2x, l2y) = sending(u), landing(u)
        half = r // 2
        src, dst, to = {
            4: (s.at[0, pl.ds(0, half), :], l1x, nx),
            5: (s.at[0, pl.ds(half, half), :], l1y, ny),
            6: (s.at[1], l2x, nx),
            7: (s.at[2], l2y, ny),
        }[k]
        return remote(src, dst, send.at[u, k], recv.at[u, k], to)

    def pair(u, q, n):
        r = rows_of(u)
        b = where[q]
        v = loading(u)
        return (
            pltpu.make_async_copy(term[u].at[pl.ds(b * r, r), :], v.at[n], lsem.at[2 * n]),
            pltpu.make_async_copy(from_peer[u].at[pl.ds((b // 2) * r, r), :], v.at[n + 2], lsem.at[2 * n + 1]),
        )

    def send_term(u):
        for k in range(4):
            copy(u, k).start()

    def fetch(u, *qs):
        copies = [c for n, q in enumerate(qs) for c in pair(u, q, n)]
        for q in qs:
            copy(u, q).wait_recv()
        for c in copies:
            c.start()
        for c in copies:
            c.wait()

    in_flight = {(k, n): None for k in (False, True) for n in (4, 5, 6, 7)}

    def sent_before(u, *ks):
        for k in ks:
            if in_flight[kind(u), k] is not None:
                copy(in_flight[kind(u), k], k).wait_send()

    def ship(u, *ks):
        for k in ks:
            copy(u, k).start()
            in_flight[kind(u), k] = u

    def chunks(u, body):
        step = 16
        lax.fori_loop(0, rows_of(u) // step, lambda i, _: (body(pl.ds(pl.multiple_of(i * step, step), step)), 0)[1], 0)

    def chunks2(u, body):
        step = 16
        lax.fori_loop(0, rows_of(u) // 2 // step, lambda i, _: (body(pl.multiple_of(i * step, step)), 0)[1], 0)

    def both(v, q, rows):
        return v[q, rows, :].astype(F32) + v[q + 2, rows, :].astype(F32)

    def pass1(u):
        fetch(u, 3)
        v, s = loading(u), sending(u)
        sent_before(u, 4, 5)

        def body(rows):
            s[0, rows, :] = both(v, 0, rows).astype(BF)

        chunks(u, body)
        ship(u, 4, 5)

    def pass2(u):
        fetch(u, 1, 2)
        v, s = loading(u), sending(u)
        l1x, l1y, _, _ = landing(u)
        sent_before(u, 6, 7)
        half = rows_of(u) // 2
        copy(u, 4).wait_recv()
        copy(u, 5).wait_recv()

        def body(at):
            low, high = pl.ds(at, 16), pl.ds(at + half, 16)
            s[1, low, :] = both(v, 0, low).astype(BF)
            s[1, high, :] = (both(v, 0, high) + l1y[low, :].astype(F32)).astype(BF)
            s[2, low, :] = (both(v, 1, low) + l1x[low, :].astype(F32)).astype(BF)
            s[2, high, :] = both(v, 1, high).astype(BF)

        chunks2(u, body)
        ship(u, 6, 7)

    def pass3(u):
        fetch(u, 0)
        v = loading(u)
        _, _, l2x, l2y = landing(u)
        copy(u, 6).wait_recv()
        copy(u, 7).wait_recv()

        n, half = UNITS[u]

        def body(rows):
            total = both(v, 0, rows) + l2x[rows, :].astype(F32) + l2y[rows, :].astype(F32)
            if kind(u):
                v[1, rows, :] = total.astype(BF)
                return
            for j in range(11):
                v[1, rows, 128 * j : 128 * j + 128] = total[:, 256 * j : 256 * j + 128].astype(BF)
                v[1, rows, H + 128 * j : H + 128 * j + 128] = total[:, 256 * j + 128 : 256 * j + 256].astype(BF)

        chunks(u, body)
        if kind(u):
            copies = [pltpu.make_async_copy(v.at[1], by_d.at[n], osem.at[0])]
        else:
            cols = pl.ds(half * H, H)
            copies = [
                pltpu.make_async_copy(v.at[1, :, pl.ds(0, H)], by_g.at[n, :, cols], osem.at[0]),
                pltpu.make_async_copy(v.at[1, :, pl.ds(H, H)], by_u.at[n, :, cols], osem.at[1]),
            ]
        for c in copies:
            c.start()
        for c in copies:
            c.wait()

    def load(src, dst, n):
        return pltpu.make_async_copy(src, dst, extra.at[n])

    def grad_gu(u, dgu):
        half = UNITS[u][1]

        def body(d_ref, out_ref):
            for m in range(0, D, 512):
                out_ref[m : m + 512, :] = dot(resident_t[m : m + 512, :], d_ref[...]).astype(BF)

        pltpu.emit_pipeline(
            body,
            grid=(11,),
            in_specs=[block(T, 256, lambda j: (0, j + 11 * half))],
            out_specs=[block(D, 256, lambda j: (0, j))],
        )(dgu, term[u])

    def grad_down(u, act):
        def body(act_ref, out_ref):
            out_ref[...] = dotg(act_ref[...], resident[...], TN).astype(BF)

        pltpu.emit_pipeline(
            body,
            grid=(11,),
            in_specs=[block(T, 256, lambda j: (0, j))],
            out_specs=[block(256, D, lambda j: (j, 0))],
        )(act, term[u])

    def grad_in(dgu, h, dh, out, first, count):
        def body(d_ref, h_ref, dh_ref, out_ref):
            da = dotg(d_ref[:, :FF], weights[0], NT) + dotg(d_ref[:, FF:], weights[1], NT)
            d = da.astype(BF).astype(F32)
            wide = h_ref[...].astype(F32)
            scale = lax.rsqrt(jnp.mean(wide * wide, -1, keepdims=True) + 1e-6)
            by_h = d * scale - wide * (scale * scale * scale * jnp.mean(d * wide, -1, keepdims=True))
            out_ref[...] = dh_ref[...] + by_h.astype(BF)

        t = lambda i: (i + first, 0)
        pltpu.emit_pipeline(
            body,
            grid=(count,),
            in_specs=[block(256, 2 * FF, t), block(256, D, t), block(256, D, t)],
            out_specs=[block(256, D, t)],
        )(dgu, h, dh, out)

    def act_back(w, gu, dgu):
        def body(w_ref, gu_ref, dgu_ref):
            for m in range(0, T, 512):
                rows = slice(m, m + 512)
                dd = dotg(resident[rows, :], w_ref[...], NT).astype(BF).astype(F32)
                for n in range(2):
                    g = gu_ref[rows, 256 * n : 256 * n + 128]
                    up = gu_ref[rows, 256 * n + 128 : 256 * n + 256]
                    d = dd[:, 128 * n : 128 * n + 128]
                    sg = sigmoid(g)
                    silu = g * sg
                    dgu_ref[rows, 256 * n : 256 * n + 128] = (d * up * (sg + silu * (1.0 - sg))).astype(BF)
                    dgu_ref[rows, 256 * n + 128 : 256 * n + 256] = (d * silu).astype(BF)

        pltpu.emit_pipeline(
            body,
            grid=(11,),
            in_specs=[block(256, D, lambda j: (j, 0)), block(T, 512, lambda j: (0, j))],
            out_specs=[block(T, 512, lambda j: (0, j))],
        )(w, gu, dgu)

    barrier((nx, ny, peer))
    loads = [load(a1t, resident_t, 0), load(dy, resident, 1), load(w10, weights.at[0], 2), load(w11, weights.at[1], 3)]
    for c in loads:
        c.start()
    loads[0].wait()
    grad_gu(4, dgu1)
    send_term(4)
    grad_gu(5, dgu1)
    send_term(5)
    again = load(a0t, resident_t, 0)
    again.start()
    pass1(4)
    loads[1].wait()
    grad_down(3, act1)
    send_term(3)
    pass2(4)
    pass1(5)
    loads[2].wait()
    loads[3].wait()
    grad_in(dgu1, h1, dy, dh1, 0, 4)
    pass2(5)
    pass1(3)
    grad_in(dgu1, h1, dy, dh1, 4, 4)
    loads = [load(dh1, resident, 1), load(w00, weights.at[0], 2), load(w01, weights.at[1], 3)]
    for c in loads:
        c.start()
    pass3(4)
    pass2(3)
    loads[0].wait()
    act_back(w02, gu0, dgu0)
    pass3(5)
    grad_down(2, act0)
    send_term(2)
    pass3(3)
    again.wait()
    grad_gu(0, dgu0)
    send_term(0)
    pass1(2)
    grad_gu(1, dgu0)
    send_term(1)
    pass2(2)
    pass1(0)
    loads[1].wait()
    loads[2].wait()
    grad_in(dgu0, x, dh1, dx, 0, 4)
    pass2(0)
    pass1(1)
    grad_in(dgu0, x, dh1, dx, 4, 4)
    pass2(1)
    pass3(2)
    pass3(0)
    pass3(1)
    for (_, k), u in in_flight.items():
        copy(u, k).wait_send()
    for u in range(6):
        for k in range(4):
            copy(u, k).wait_send()


def backward(x, dy, saved):
    full, (_, a0t, h1, _, a1t, act0, gu0, act1, dgu1, _) = saved[:6], saved[6:]
    any_ = pl.BlockSpec(memory_space=ANY)
    s = jax.ShapeDtypeStruct
    outs = [s((2, GROWS, FF), BF)] * 2 + [s((2, DROWS, D), BF)]
    outs += [s((T, D), BF), s((T, D), BF), s((T, 2 * FF), BF)]
    outs += [s(full_shape(u), BF) for u in range(6)]
    outs += [s((4 * rows_of(u), full_shape(u)[1]), BF) for u in range(6)]
    dma = pltpu.SemaphoreType.DMA
    return pl.pallas_call(
        backward_kernel,
        out_shape=outs,
        in_specs=[any_] * 14,
        out_specs=[any_] * len(outs),
        scratch_shapes=[
            VMEM((2, D, FF), BF),
            VMEM((T, D), BF),
            VMEM((D, T), BF),
            *[VMEM((4, GROWS // 2, FF), BF)] * 2,
            *[VMEM((4, GROWS, FF), BF)] * 2,
            *[VMEM((2, DROWS // 2, D), BF)] * 2,
            *[VMEM((2, DROWS, D), BF)] * 2,
            VMEM((3, GROWS, FF), BF),
            VMEM((3, DROWS, D), BF),
            VMEM((4, GROWS, FF), BF),
            VMEM((4, DROWS, D), BF),
            dma((6, 8)),
            dma((6, 8)),
            dma((4,)),
            dma((4,)),
            dma((2,)),
        ],
        compiler_params=pltpu.CompilerParams(collective_id=1, has_side_effects=True, vmem_limit_bytes=63 * MIB),
        name="backward_scatter",
    )(x, h1, dy, a0t, a1t, act0, act1, gu0, dgu1, full[0], full[1], full[2], full[4], full[5])


def solution(mesh):
    def body(x, dy, wg, wu, wd):
        x, dy = x[0], dy[0]
        saved = forward(x, dy, wg, wu, wd)
        by_g, by_u, by_d, dx = backward(x, dy, saved)[:4]
        return dx[None], by_g, by_u, by_d

    seq, rows = P(("rep", "dp"), None, None), P(None, "dp", None)
    out = P("rep", "dp", None)
    return jax.shard_map(body, mesh=mesh, in_specs=(seq, seq, rows, rows, rows), out_specs=(seq, out, out, out), check_vma=False)
```

```python
import jax
import jax.numpy as jnp
from jax import lax
from jax.experimental import pallas as pl
from jax.experimental.pallas import tpu as pltpu
from jax.sharding import PartitionSpec as P

BF, F32 = jnp.bfloat16, jnp.float32
T, D, FF = 2048, 1024, 2816
H = FF // 2
GROWS, DROWS = D // 8, FF // 8
UNITS = ((0, 0), (0, 1), (0, 2), (1, 2), (1, 0), (1, 1))
NT = (((1,), (1,)), ((), ()))
TN = (((0,), (0,)), ((), ()))
VMEM = pltpu.VMEM
ANY = pl.ANY
L, W, M = 128, 256, 512
STEPS = FF // W


def rows_of(u):
    return DROWS if UNITS[u][1] == 2 else GROWS


def full_shape(u):
    return (FF, D) if UNITS[u][1] == 2 else (D, FF)


def sigmoid(z):
    return 0.5 * jnp.tanh(0.5 * z) + 0.5


def dot(a, b):
    return jnp.dot(a, b, preferred_element_type=F32)


def dotg(a, b, dims):
    return lax.dot_general(a, b, dims, preferred_element_type=F32)


def places():
    me = lax.axis_index("dp")
    ix, iy, ic = me // 4, (me // 2) % 2, me % 2
    flip = lambda a, b, c: (ix + a - 2 * a * ix) * 4 + (iy + b - 2 * b * iy) * 2 + (ic + c - 2 * c * ic)
    return me, flip


def barrier(peers):
    sem = pltpu.get_barrier_semaphore()
    for p in peers:
        pl.semaphore_signal(sem, inc=1, device_id={"dp": p}, device_id_type=pl.DeviceIdType.MESH)
    pl.semaphore_wait(sem, len(peers))


def remote(src, dst, send, recv, to):
    return pltpu.make_async_remote_copy(src_ref=src, dst_ref=dst, send_sem=send, recv_sem=recv, device_id={"dp": to}, device_id_type=pl.DeviceIdType.MESH)


def block(rows, cols, index):
    return pl.BlockSpec((rows, cols), index)


def row(i):
    return i, 0


def col(j):
    return 0, j


def pipeline(body, grid, ins, outs, hooks, *arrays):
    def run(*refs):
        step = pl.program_id(0)
        if len(grid) == 2:
            step = step * grid[1] + pl.program_id(1)
        for at, work in (hooks or {}).items():
            pl.when(step == at)(work)
        body(*refs)

    pltpu.emit_pipeline(run, grid=grid, in_specs=ins, out_specs=outs)(*arrays)


def inverse_rms(wide):
    return lax.rsqrt(jnp.mean(wide * wide, -1, keepdims=True) + 1e-6)


def kernel(x, dy, wg, wu, wd, *refs):
    (by_g, by_u, by_d, dx), refs = refs[:4], refs[4:]
    full, term, from_peer, refs = refs[:6], refs[6:12], refs[12:18], refs[18:]
    a0, a0t, h1, a1, a1t, act0, gu0, act1, dgu1, dact1, dh1, dgu0, refs = *refs[:12], refs[12:]
    weights, down, resident, resident_t, *landings, gsend, dsend, gload, dload, gsem, gsem2, send, recv, local, mix, extra, lsem, osem = refs
    me, flip = places()
    nx, ny, peer, nxy = flip(1, 0, 0), flip(0, 1, 0), flip(0, 0, 1), flip(1, 1, 0)
    shards = [wd.at[n] if part == 2 else gload.at[2 * n + part] for n, part in UNITS]

    def load(src, dst, n):
        return pltpu.make_async_copy(src, dst, extra.at[n])


    def part(u, b, half=None):
        r = rows_of(u)
        if half is None:
            return full[u].at[pl.ds(b * r, r), :]
        return full[u].at[pl.ds(b * r + half * (r // 2), r // 2), :]

    def hop(u, k):
        src, dst, to = (
            (shards[u], part(u, me), nx),
            (shards[u], part(u, me), ny),
            (shards[u], part(u, me), peer),
            (part(u, nx, 0), part(u, nx, 0), ny),
            (part(u, ny, 1), part(u, ny, 1), nx),
            (part(u, nx), part(u, nx), peer),
            (part(u, ny), part(u, ny), peer),
            (part(u, nxy, 0), part(u, nxy, 0), peer),
            (part(u, nxy, 1), part(u, nxy, 1), peer),
        )[k]
        return remote(src, dst, gsem.at[u, k], gsem2.at[u, k], to)

    def own_copy(u):
        return pltpu.make_async_copy(shards[u], part(u, me), local.at[u])

    def start_own(u):
        for k in range(3):
            hop(u, k).start()
        own_copy(u).start()

    def pass_on(u):
        for k in (0, 1):
            hop(u, k).wait_recv()
            hop(u, k + 3).start()
            hop(u, k + 5).start()

    def pass_on_last(u):
        for k in (3, 4):
            hop(u, k).wait_recv()
            hop(u, k + 4).start()

    def arrived(u):
        own_copy(u).wait()
        for k in (2, 5, 6, 7, 8):
            hop(u, k).wait_recv()

    def mix_start(u):
        n, half = UNITS[u]
        for j in range(STEPS):
            cols = pl.ds(half * H + L * j, L)
            for i, w in enumerate((wg, wu)):
                pltpu.make_async_copy(w.at[n, :, cols], shards[u].at[:, pl.ds(W * j + L * i, L)], mix.at[u]).start()

    def mix_wait(u):
        pltpu.make_async_copy(shards[u], shards[u], mix.at[u]).wait()

    where = (me, nx, ny, nxy)

    def kind(u):
        return UNITS[u][1] == 2

    slot = (0, 1, 0, 1, 2, 3)
    before = {5: 4, 0: 5, 1: 0, 2: 3}

    def landing(u):
        return tuple(t.at[slot[u]] for t in landings[4 * kind(u) : 4 * kind(u) + 4])

    def sending(u):
        return dsend if kind(u) else gsend

    def loading(u):
        return dload if kind(u) else gload

    def copy(u, k):
        r = rows_of(u)
        if k < 4:
            b = where[k]
            other = b + 1 - 2 * (b % 2)
            return remote(term[u].at[pl.ds(other * r, r), :], from_peer[u].at[pl.ds((b // 2) * r, r), :], send.at[u, k], recv.at[u, k], peer)
        s, (l1x, l1y, l2x, l2y) = sending(u), landing(u)
        half = r // 2
        src, dst, to = (
            (s.at[0, pl.ds(0, half), :], l1x, nx),
            (s.at[0, pl.ds(half, half), :], l1y, ny),
            (s.at[1], l2x, nx),
            (s.at[2], l2y, ny),
        )[k - 4]
        return remote(src, dst, send.at[u, k], recv.at[u, k], to)

    def send_term(u):
        for k in (3, 1, 2, 0):
            copy(u, k).start()

    def pairs(u, qs):
        r, v = rows_of(u), loading(u)
        for n, q in enumerate(qs):
            b = where[q]
            yield pltpu.make_async_copy(term[u].at[pl.ds(b * r, r), :], v.at[n], lsem.at[2 * n])
            yield pltpu.make_async_copy(from_peer[u].at[pl.ds((b // 2) * r, r), :], v.at[n + 2], lsem.at[2 * n + 1])

    def fetch(u, *qs):
        for q in qs:
            copy(u, q).wait_recv()
        for c in pairs(u, qs):
            c.start()

    def fetched(u, *qs):
        for c in pairs(u, qs):
            c.wait()

    def chunks(count, body):
        def step(i, _):
            body(pl.multiple_of(i * 16, 16))
            return 0

        lax.fori_loop(0, count // 16, step, 0)

    def both(v, n, rows):
        return v[n, rows, :].astype(F32) + v[n + 2, rows, :].astype(F32)

    def sent_before(u, *ks):
        if u in before:
            for k in ks:
                copy(before[u], k).wait_send()

    def fetch1(u):
        return lambda: fetch(u, 3)

    def fetch2(u):
        return lambda: fetch(u, 1, 2)

    def fetch3(u):
        return lambda: fetch(u, 0)

    def pass1(u):
        def work():
            fetched(u, 3)
            v, s = loading(u), sending(u)
            sent_before(u, 4, 5)

            def body(at):
                rows = pl.ds(at, 16)
                s[0, rows, :] = both(v, 0, rows).astype(BF)

            chunks(rows_of(u), body)
            copy(u, 4).start()
            copy(u, 5).start()

        return work

    def pass2(u):
        def work():
            fetched(u, 1, 2)
            v, s = loading(u), sending(u)
            l1x, l1y, _, _ = landing(u)
            sent_before(u, 6, 7)
            half = rows_of(u) // 2
            copy(u, 4).wait_recv()
            copy(u, 5).wait_recv()

            def body(at):
                low, high = pl.ds(at, 16), pl.ds(at + half, 16)
                s[1, low, :] = both(v, 0, low).astype(BF)
                s[1, high, :] = (both(v, 0, high) + l1y[low, :].astype(F32)).astype(BF)
                s[2, low, :] = (both(v, 1, low) + l1x[low, :].astype(F32)).astype(BF)
                s[2, high, :] = both(v, 1, high).astype(BF)

            chunks(half, body)
            copy(u, 6).start()
            copy(u, 7).start()

        return work

    def pass3(u):
        def work():
            fetched(u, 0)
            v = loading(u)
            _, _, l2x, l2y = landing(u)
            copy(u, 6).wait_recv()
            copy(u, 7).wait_recv()
            n, half = UNITS[u]

            def body(at):
                rows = pl.ds(at, 16)
                total = (both(v, 0, rows) + l2x[rows, :].astype(F32) + l2y[rows, :].astype(F32)).astype(BF)
                if kind(u):
                    v[1, rows, :] = total
                    return
                for j in range(STEPS):
                    for i in range(2):
                        v[1, rows, H * i + L * j : H * i + L * j + L] = total[:, W * j + L * i : W * j + L * i + L]

            chunks(rows_of(u), body)
            if kind(u):
                copies = [pltpu.make_async_copy(v.at[1], by_d.at[n], osem.at[0])]
            else:
                cols = pl.ds(half * H, H)
                copies = [pltpu.make_async_copy(v.at[1, :, pl.ds(H * i, H)], t.at[n, :, cols], osem.at[i]) for i, t in enumerate((by_g, by_u))]
            for c in copies:
                c.start()
            for c in copies:
                c.wait()

        return work

    def together(*works):
        def work():
            for w in works:
                w()

        return work


    def norm_into(wide, a_ref, at_ref):
        a = (wide * inverse_rms(wide)).astype(BF)
        a_ref[...] = a
        at_ref[...] = a.T

    def norm_body(x_ref, a_ref, at_ref):
        norm_into(x_ref[...].astype(F32), a_ref, at_ref)

    def gate_up0(half):
        def body(w_ref, gu_ref, act_ref):
            for m in range(0, T, M):
                s = dot(resident[m : m + M, :], w_ref[...])
                gu_ref[m : m + M, :] = s
                g, up = s[:, :L], s[:, L:]
                act_ref[m : m + M, :] = (g * sigmoid(g) * up).astype(BF)

        cols = lambda j: (0, j + STEPS * half)
        pipeline(body, (STEPS,), [block(D, W, col)], [block(T, W, cols), block(T, L, cols)], None, full[half], gu0, act0)

    def down_body(act_ref, x_ref, h_ref, a_ref, at_ref):
        h = x_ref[...] + dot(act_ref[...], down[...]).astype(BF)
        h_ref[...] = h
        norm_into(h.astype(F32), a_ref, at_ref)

    def dact_body(w_ref, out_ref):
        for m in range(0, T, M):
            out_ref[m : m + M, :] = dotg(resident[m : m + M, :], w_ref[...], NT).astype(BF)

    def back(g, up, d):
        sg = sigmoid(g)
        silu = g * sg
        return silu, (d * up * (sg + silu * (1.0 - sg))).astype(BF), (d * silu).astype(BF)

    def gate_up1(half, hooks):
        def body(w_ref, dact_ref, act_ref, dgu_ref):
            for m in range(0, T, M):
                rows = slice(m, m + M)
                s = dot(resident[rows, :], w_ref[...])
                up = s[:, L:]
                silu, dg, du = back(s[:, :L], up, dact_ref[rows, :].astype(F32))
                act_ref[rows, :] = (silu * up).astype(BF)
                dgu_ref[rows, :L] = dg
                dgu_ref[rows, L:] = du

        cols = lambda j: (0, j + STEPS * half)
        ins, outs = [block(D, W, col), block(T, L, cols)], [block(T, L, cols), block(T, W, cols)]
        pipeline(body, (STEPS,), ins, outs, hooks, full[4 + half], dact1, act1, dgu1)

    def grad_gu(u, dgu, hooks):
        half = UNITS[u][1]

        def body(d_ref, out_ref):
            for m in range(0, D, M):
                out_ref[m : m + M, :] = dot(resident_t[m : m + M, :], d_ref[...]).astype(BF)

        pipeline(body, (STEPS,), [block(T, W, lambda j: (0, j + STEPS * half))], [block(D, W, col)], hooks, dgu, term[u])
        send_term(u)

    def grad_down(u, act, hooks):
        def body(act_ref, out_ref):
            out_ref[...] = dotg(act_ref[...], resident[...], TN).astype(BF)

        pipeline(body, (STEPS,), [block(T, W, col)], [block(W, D, row)], hooks, act, term[u])
        send_term(u)

    def grad_in(dgu, h, dh, out, keep, hooks):
        def body(d_ref, h_ref, dh_ref, out_ref):
            da = dotg(d_ref[:, :FF], weights[0], NT) + dotg(d_ref[:, FF:], weights[1], NT)
            d = da.astype(BF).astype(F32)
            wide = h_ref[...].astype(F32)
            scale = inverse_rms(wide)
            by_h = d * scale - wide * (scale * scale * scale * jnp.mean(d * wide, -1, keepdims=True))
            total = dh_ref[...] + by_h.astype(BF)
            out_ref[...] = total
            if keep:
                resident[pl.ds(pl.multiple_of(pl.program_id(0) * W, W), W), :] = total

        pipeline(body, (T // W,), [block(W, 2 * FF, row)] + [block(W, D, row)] * 2, [block(W, D, row)], hooks, dgu, h, dh, out)

    def act_back(hooks):
        def body(w_ref, gu_ref, dgu_ref):
            first = pl.program_id(0) * (T // 2)
            for m in range(0, T // 2, M):
                rows = slice(m, m + M)
                dd = dotg(resident[pl.ds(pl.multiple_of(first + m, M), M), :], w_ref[...], NT).astype(BF).astype(F32)
                for n in range(2):
                    at = W * n
                    _, dg, du = back(gu_ref[rows, at : at + L], gu_ref[rows, at + L : at + W], dd[:, L * n : L * n + L])
                    dgu_ref[rows, at : at + L] = dg
                    dgu_ref[rows, at + L : at + W] = du

        wide = block(T // 2, M, lambda i, j: (i, j))
        pipeline(body, (2, STEPS), [block(W, D, lambda i, j: (j, 0)), wide], [wide], hooks, full[2], gu0, dgu0)

    for u in (0, 1, 4, 5):
        mix_start(u)
    barrier((nx, ny, peer))
    for u in range(2):
        mix_wait(u)
        start_own(u)
    mix_wait(4)
    mix_wait(5)
    pipeline(norm_body, (T // W,), [block(W, D, row)], [block(W, D, row), block(D, W, col)], None, x, a0, a0t)
    in_a = load(a0, resident, 0)
    in_a.start()
    pass_on(0)
    start_own(2)
    pass_on_last(0)
    pass_on(1)
    start_own(3)
    arrived(0)
    in_a.wait()
    gate_up0(0)
    pass_on_last(1)
    pass_on(2)
    start_own(4)
    arrived(1)
    gate_up0(1)
    in_dy = load(dy, resident, 0)
    in_dy.start()
    pass_on_last(2)
    pass_on(3)
    start_own(5)
    arrived(2)
    in_down = load(full[2], down, 1)
    in_down.start()
    in_down.wait()
    outs = [block(M, D, row), block(M, D, row), block(D, M, col)]
    pipeline(down_body, (T // M,), [block(M, FF, row), block(M, D, row)], outs, None, act0, x, h1, a1, a1t)
    in_at = load(a1t, resident_t, 1)
    in_at.start()
    in_dy.wait()
    pass_on_last(3)
    pass_on(4)
    arrived(3)
    pipeline(dact_body, (STEPS,), [block(W, D, row)], [block(T, W, col)], None, full[3], dact1)
    in_a = load(a1, resident, 0)
    in_a.start()
    pass_on_last(4)
    in_at.wait()
    in_a.wait()
    arrived(4)
    gate_up1(0, {5: lambda: pass_on(5)})
    grad_gu(4, dgu1, None)
    pass_on_last(5)
    arrived(5)
    for u in range(6):
        for k in range(9):
            hop(u, k).wait_send()
    in_w = [load(full[4 + i], weights.at[i], 2 + i) for i in range(2)]
    for c in in_w:
        c.start()
    gate_up1(1, {4: fetch1(4), 6: pass1(4)})
    in_dy = load(dy, resident, 0)
    in_dy.start()
    grad_gu(5, dgu1, {1: fetch2(4), 4: pass2(4)})
    in_at = load(a0t, resident_t, 1)
    in_at.start()
    in_dy.wait()
    grad_down(3, act1, {4: fetch1(5), 6: pass1(5), 7: fetch3(4), 9: pass3(4)})
    for c in in_w:
        c.wait()
    grad_in(dgu1, h1, dy, dh1, True, {0: fetch2(5), 1: together(pass2(5), fetch1(3)), 3: pass1(3), 6: fetch3(5), 7: pass3(5)})
    in_w = [load(full[i], weights.at[i], 2 + i) for i in range(2)]
    for c in in_w:
        c.start()
    grad_down(2, act0, {0: fetch2(3), 2: pass2(3)})
    act_back({4: fetch3(3), 7: together(pass3(3), fetch1(2)), 10: pass1(2)})
    in_at.wait()
    grad_gu(0, dgu0, {0: fetch2(2), 2: pass2(2)})
    grad_gu(1, dgu0, {4: fetch1(0), 6: pass1(0), 7: fetch3(2), 10: pass3(2)})
    for c in in_w:
        c.wait()
    grad_in(dgu0, x, dh1, dx, False, {0: fetch2(0), 1: together(pass2(0), fetch1(1)), 2: pass1(1), 6: fetch3(0), 7: together(pass3(0), fetch2(1))})
    pass2(1)()
    fetch3(1)()
    pass3(1)()
    for u in (1, 2):
        for k in range(4, 8):
            copy(u, k).wait_send()
    for u in range(6):
        for k in range(4):
            copy(u, k).wait_send()


def solution(mesh):
    any_ = pl.BlockSpec(memory_space=ANY)
    dma = pltpu.SemaphoreType.DMA

    def s(*shape, dtype=BF):
        return jax.ShapeDtypeStruct(shape, dtype)

    outs = [s(2, GROWS, FF), s(2, GROWS, FF), s(2, DROWS, D), s(T, D)]
    outs += [s(*full_shape(u)) for u in range(6)] * 2
    outs += [s(4 * rows_of(u), full_shape(u)[1]) for u in range(6)]
    outs += [s(T, D), s(D, T), s(T, D), s(T, D), s(D, T), s(T, FF), s(T, 2 * FF, dtype=F32), s(T, FF), s(T, 2 * FF), s(T, FF), s(T, D), s(T, 2 * FF)]
    scratch = [VMEM((2, D, FF), BF), VMEM((FF, D), BF), VMEM((T, D), BF), VMEM((D, T), BF)]
    scratch += [VMEM((4, r, FF), BF) for r in (GROWS // 2, GROWS // 2, GROWS, GROWS)]
    scratch += [VMEM((2, r, D), BF) for r in (DROWS // 2, DROWS // 2, DROWS, DROWS)]
    scratch += [VMEM((3, GROWS, FF), BF), VMEM((3, DROWS, D), BF), VMEM((4, GROWS, FF), BF), VMEM((4, DROWS, D), BF)]
    scratch += [dma((6, 9)), dma((6, 9)), dma((6, 8)), dma((6, 8)), dma((6,)), dma((6,)), dma((4,)), dma((4,)), dma((2,))]
    step = pl.pallas_call(
        kernel,
        out_shape=outs,
        in_specs=[any_] * 4 + [pl.BlockSpec(memory_space=VMEM)],
        out_specs=[any_] * len(outs),
        scratch_shapes=scratch,
        compiler_params=pltpu.CompilerParams(collective_id=0, has_side_effects=True, vmem_limit_bytes=63 << 20),
        name="step",
    )

    def body(x, dy, wg, wu, wd):
        by_g, by_u, by_d, dx = step(x[0], dy[0], wg, wu, wd)[:4]
        return dx[None], by_g, by_u, by_d

    seq, rows = P(("rep", "dp"), None, None), P(None, "dp", None)
    out = P("rep", "dp", None)
    return jax.shard_map(body, mesh=mesh, in_specs=(seq, seq, rows, rows, rows), out_specs=(seq, out, out, out), check_vma=False)
```

```python
import jax
import jax.numpy as jnp
from jax import lax
from jax.experimental import pallas as pl
from jax.experimental.pallas import tpu as pltpu
from jax.sharding import PartitionSpec as P

BF, F32 = jnp.bfloat16, jnp.float32
T, D, FF = 2048, 1024, 2816
H = FF // 2
GROWS, DROWS = D // 8, FF // 8
UNITS = ((0, 0), (0, 1), (0, 2), (1, 2), (1, 0), (1, 1))
NT = (((1,), (1,)), ((), ()))
TN = (((0,), (0,)), ((), ()))
VMEM = pltpu.VMEM
ANY = pl.ANY
L, W, M = 128, 256, 512
STEPS = FF // W


def rows_of(u):
    return DROWS if UNITS[u][1] == 2 else GROWS


def full_shape(u):
    return (FF, D) if UNITS[u][1] == 2 else (D, FF)


def sigmoid(z):
    return 0.5 * jnp.tanh(0.5 * z) + 0.5


def dot(a, b):
    return jnp.dot(a, b, preferred_element_type=F32)


def dotg(a, b, dims):
    return lax.dot_general(a, b, dims, preferred_element_type=F32)


def places():
    me = lax.axis_index("dp")
    ix, iy, ic = me // 4, (me // 2) % 2, me % 2
    flip = lambda a, b, c: (ix + a - 2 * a * ix) * 4 + (iy + b - 2 * b * iy) * 2 + (ic + c - 2 * c * ic)
    return me, flip


def barrier(peers):
    sem = pltpu.get_barrier_semaphore()
    for p in peers:
        pl.semaphore_signal(sem, inc=1, device_id={"dp": p}, device_id_type=pl.DeviceIdType.MESH)
    pl.semaphore_wait(sem, len(peers))


def remote(src, dst, send, recv, to):
    return pltpu.make_async_remote_copy(src_ref=src, dst_ref=dst, send_sem=send, recv_sem=recv, device_id={"dp": to}, device_id_type=pl.DeviceIdType.MESH)


def block(rows, cols, index):
    return pl.BlockSpec((rows, cols), index)


def deep(rows, cols, index):
    return pl.BlockSpec((rows, cols), index, pipeline_mode=pl.Buffered(3))


def row(i):
    return i, 0


def col(j):
    return 0, j


def pipeline(body, grid, ins, outs, hooks, *arrays):
    def run(*refs):
        step = pl.program_id(0)
        if len(grid) == 2:
            step = step * grid[1] + pl.program_id(1)
        for at, work in (hooks or {}).items():
            pl.when(step == at)(work)
        body(*refs)

    pltpu.emit_pipeline(run, grid=grid, in_specs=ins, out_specs=outs)(*arrays)


def inverse_rms(wide):
    return lax.rsqrt(jnp.mean(wide * wide, -1, keepdims=True) + 1e-6)


def kernel(x, dy, wg, wu, wd, *refs):
    (by_g, by_u, by_d, dx), refs = refs[:4], refs[4:]
    full, term, from_peer, refs = refs[:6], refs[6:12], refs[12:18], refs[18:]
    a0, a0t, h1, a1, a1t, act0, gu0, act1, dgu1, dact1, dh1, dgu0, refs = *refs[:12], refs[12:]
    weights, resident, resident_t, *landings, gsend, dsend, gload, dload, gsem, gsem2, send, recv, local, mix, extra, lsem, osem = refs
    me, flip = places()
    nx, ny, peer, nxy = flip(1, 0, 0), flip(0, 1, 0), flip(0, 0, 1), flip(1, 1, 0)
    shards = [wd.at[n] if part == 2 else gload.at[2 * n + part] for n, part in UNITS]

    def load(src, dst, n):
        return pltpu.make_async_copy(src, dst, extra.at[n])


    def part(u, b, half=None):
        r = rows_of(u)
        if half is None:
            return full[u].at[pl.ds(b * r, r), :]
        return full[u].at[pl.ds(b * r + half * (r // 2), r // 2), :]

    def hop(u, k):
        src, dst, to = (
            (shards[u], part(u, me), nx),
            (shards[u], part(u, me), ny),
            (shards[u], part(u, me), peer),
            (part(u, nx, 0), part(u, nx, 0), ny),
            (part(u, ny, 1), part(u, ny, 1), nx),
            (part(u, nx), part(u, nx), peer),
            (part(u, ny), part(u, ny), peer),
            (part(u, nxy, 0), part(u, nxy, 0), peer),
            (part(u, nxy, 1), part(u, nxy, 1), peer),
        )[k]
        return remote(src, dst, gsem.at[u, k], gsem2.at[u, k], to)

    def own_copy(u):
        return pltpu.make_async_copy(shards[u], part(u, me), local.at[u])

    def start_own(u):
        for k in range(3):
            hop(u, k).start()
        own_copy(u).start()

    def pass_on(u):
        for k in (0, 1):
            hop(u, k).wait_recv()
            hop(u, k + 3).start()
            hop(u, k + 5).start()

    def pass_on_last(u):
        for k in (3, 4):
            hop(u, k).wait_recv()
            hop(u, k + 4).start()

    def arrived(u):
        own_copy(u).wait()
        for k in (2, 5, 6, 7, 8):
            hop(u, k).wait_recv()

    def mix_start(u):
        n, half = UNITS[u]
        for j in range(STEPS):
            cols = pl.ds(half * H + L * j, L)
            for i, w in enumerate((wg, wu)):
                pltpu.make_async_copy(w.at[n, :, cols], shards[u].at[:, pl.ds(W * j + L * i, L)], mix.at[u]).start()

    def mix_wait(u):
        pltpu.make_async_copy(shards[u], shards[u], mix.at[u]).wait()

    where = (me, nx, ny, nxy)

    def kind(u):
        return UNITS[u][1] == 2

    slot = (0, 1, 0, 1, 2, 3)
    before = {5: 4, 0: 5, 1: 0, 2: 3}

    def landing(u):
        return tuple(t.at[slot[u]] for t in landings[4 * kind(u) : 4 * kind(u) + 4])

    def sending(u):
        return dsend if kind(u) else gsend

    def loading(u):
        return dload if kind(u) else gload

    def copy(u, k):
        r = rows_of(u)
        if k < 4:
            b = where[k]
            other = b + 1 - 2 * (b % 2)
            return remote(term[u].at[pl.ds(other * r, r), :], from_peer[u].at[pl.ds((b // 2) * r, r), :], send.at[u, k], recv.at[u, k], peer)
        s, (l1x, l1y, l2x, l2y) = sending(u), landing(u)
        half = r // 2
        src, dst, to = (
            (s.at[0, pl.ds(0, half), :], l1x, nx),
            (s.at[0, pl.ds(half, half), :], l1y, ny),
            (s.at[1], l2x, nx),
            (s.at[2], l2y, ny),
        )[k - 4]
        return remote(src, dst, send.at[u, k], recv.at[u, k], to)

    def send_term(u):
        for k in (3, 1, 2, 0):
            copy(u, k).start()

    def pairs(u, qs):
        r, v = rows_of(u), loading(u)
        for n, q in enumerate(qs):
            b = where[q]
            yield pltpu.make_async_copy(term[u].at[pl.ds(b * r, r), :], v.at[n], lsem.at[2 * n])
            yield pltpu.make_async_copy(from_peer[u].at[pl.ds((b // 2) * r, r), :], v.at[n + 2], lsem.at[2 * n + 1])

    def fetch(u, *qs):
        for q in qs:
            copy(u, q).wait_recv()
        for c in pairs(u, qs):
            c.start()

    def fetched(u, *qs):
        for c in pairs(u, qs):
            c.wait()

    def chunks(count, body):
        def step(i, _):
            body(pl.multiple_of(i * 16, 16))
            return 0

        lax.fori_loop(0, count // 16, step, 0)

    def both(v, n, rows):
        return v[n, rows, :].astype(F32) + v[n + 2, rows, :].astype(F32)

    def sent_before(u, *ks):
        if u in before:
            for k in ks:
                copy(before[u], k).wait_send()

    def fetch1(u):
        return lambda: fetch(u, 3)

    def fetch2(u):
        return lambda: fetch(u, 1, 2)

    def fetch3(u):
        return lambda: fetch(u, 0)

    def pass1(u):
        def work():
            fetched(u, 3)
            v, s = loading(u), sending(u)
            sent_before(u, 4, 5)

            def body(at):
                rows = pl.ds(at, 16)
                s[0, rows, :] = both(v, 0, rows).astype(BF)

            chunks(rows_of(u), body)
            copy(u, 4).start()
            copy(u, 5).start()

        return work

    def pass2(u):
        def work():
            fetched(u, 1, 2)
            v, s = loading(u), sending(u)
            l1x, l1y, _, _ = landing(u)
            sent_before(u, 6, 7)
            half = rows_of(u) // 2
            copy(u, 4).wait_recv()
            copy(u, 5).wait_recv()

            def body(at):
                low, high = pl.ds(at, 16), pl.ds(at + half, 16)
                s[1, low, :] = both(v, 0, low).astype(BF)
                s[1, high, :] = (both(v, 0, high) + l1y[low, :].astype(F32)).astype(BF)
                s[2, low, :] = (both(v, 1, low) + l1x[low, :].astype(F32)).astype(BF)
                s[2, high, :] = both(v, 1, high).astype(BF)

            chunks(half, body)
            copy(u, 6).start()
            copy(u, 7).start()

        return work

    def pass3(u):
        def work():
            fetched(u, 0)
            v = loading(u)
            _, _, l2x, l2y = landing(u)
            copy(u, 6).wait_recv()
            copy(u, 7).wait_recv()
            n, half = UNITS[u]

            def body(at):
                rows = pl.ds(at, 16)
                total = (both(v, 0, rows) + l2x[rows, :].astype(F32) + l2y[rows, :].astype(F32)).astype(BF)
                if kind(u):
                    v[1, rows, :] = total
                    return
                for j in range(STEPS):
                    for i in range(2):
                        v[1, rows, H * i + L * j : H * i + L * j + L] = total[:, W * j + L * i : W * j + L * i + L]

            chunks(rows_of(u), body)
            if kind(u):
                copies = [pltpu.make_async_copy(v.at[1], by_d.at[n], osem.at[0])]
            else:
                cols = pl.ds(half * H, H)
                copies = [pltpu.make_async_copy(v.at[1, :, pl.ds(H * i, H)], t.at[n, :, cols], osem.at[i]) for i, t in enumerate((by_g, by_u))]
            for c in copies:
                c.start()
            for c in copies:
                c.wait()

        return work

    def together(*works):
        def work():
            for w in works:
                w()

        return work


    def norm_into(wide, a_ref, at_ref):
        a = (wide * inverse_rms(wide)).astype(BF)
        a_ref[...] = a
        at_ref[...] = a.T

    def norm_body(x_ref, a_ref, at_ref):
        norm_into(x_ref[...].astype(F32), a_ref, at_ref)

    def gate_up0(half):
        def body(w_ref, gu_ref, act_ref):
            for m in range(0, T, M):
                s = dot(resident[m : m + M, :], w_ref[...])
                gu_ref[m : m + M, :] = s
                g, up = s[:, :L], s[:, L:]
                act_ref[m : m + M, :] = (g * sigmoid(g) * up).astype(BF)

        cols = lambda j: (0, j + STEPS * half)
        tiles = pl.BlockSpec((None, T, W), lambda j: (j + STEPS * half, 0, 0))
        pipeline(body, (STEPS,), [block(D, W, col)], [tiles, block(T, L, cols)], None, full[half], gu0, act0)

    def down_op(down, sem):
        in_down = pltpu.make_async_copy(full[2], down, sem)
        in_down.start()
        in_down.wait()

        def body(act_ref, x_ref, h_ref, a_ref, at_ref):
            h = x_ref[...] + dot(act_ref[...], down[...]).astype(BF)
            h_ref[...] = h
            norm_into(h.astype(F32), a_ref, at_ref)

        outs = [block(M, D, row), block(M, D, row), block(D, M, col)]
        pipeline(body, (T // M,), [block(M, FF, row), block(M, D, row)], outs, None, act0, x, h1, a1, a1t)

    def dact_body(w_ref, out_ref):
        for m in range(0, T, M):
            out_ref[m : m + M, :] = dotg(resident[m : m + M, :], w_ref[...], NT).astype(BF)

    def back(g, up, d):
        sg = sigmoid(g)
        silu = g * sg
        return silu, (d * up * (sg + silu * (1.0 - sg))).astype(BF), (d * silu).astype(BF)

    def gate_up1(half, hooks):
        def body(w_ref, dact_ref, act_ref, dgu_ref):
            for m in range(0, T, M):
                rows = slice(m, m + M)
                s = dot(resident[rows, :], w_ref[...])
                up = s[:, L:]
                silu, dg, du = back(s[:, :L], up, dact_ref[rows, :].astype(F32))
                act_ref[rows, :] = (silu * up).astype(BF)
                dgu_ref[rows, :L] = dg
                dgu_ref[rows, L:] = du

        cols = lambda j: (0, j + STEPS * half)
        ins, outs = [block(D, W, col), block(T, L, cols)], [block(T, L, cols), block(T, W, cols)]
        pipeline(body, (STEPS,), ins, outs, hooks, full[4 + half], dact1, act1, dgu1)

    def grad_gu(u, dgu, hooks):
        half = UNITS[u][1]

        def body(d_ref, out_ref):
            for m in range(0, D, M):
                out_ref[m : m + M, :] = dot(resident_t[m : m + M, :], d_ref[...]).astype(BF)

        pipeline(body, (STEPS,), [deep(T, W, lambda j: (0, j + STEPS * half))], [block(D, W, col)], hooks, dgu, term[u])
        send_term(u)

    def grad_down(u, act, hooks):
        def body(act_ref, out_ref):
            out_ref[...] = dotg(act_ref[...], resident[...], TN).astype(BF)

        pipeline(body, (STEPS,), [deep(T, W, col)], [block(W, D, row)], hooks, act, term[u])
        send_term(u)

    def grad_in(dgu, h, dh, out, keep, hooks):
        def body(d_ref, h_ref, dh_ref, out_ref):
            da = dotg(d_ref[:, :FF], weights[0], NT) + dotg(d_ref[:, FF:], weights[1], NT)
            d = da.astype(BF).astype(F32)
            wide = h_ref[...].astype(F32)
            scale = inverse_rms(wide)
            by_h = d * scale - wide * (scale * scale * scale * jnp.mean(d * wide, -1, keepdims=True))
            total = dh_ref[...] + by_h.astype(BF)
            out_ref[...] = total
            if keep:
                resident[pl.ds(pl.multiple_of(pl.program_id(0) * W, W), W), :] = total

        pipeline(body, (T // W,), [block(W, 2 * FF, row)] + [block(W, D, row)] * 2, [block(W, D, row)], hooks, dgu, h, dh, out)

    def act_back(u, hooks):
        def body(w_ref, gu_ref, dgu_ref, out_ref):
            for m in range(0, T, M):
                rows = slice(m, m + M)
                dd = dotg(resident[rows, :], w_ref[...], NT).astype(BF).astype(F32)
                for n in range(2):
                    at, up = W * n, gu_ref[n, rows, L:]
                    silu, dg, du = back(gu_ref[n, rows, :L], up, dd[:, L * n : L * n + L])
                    dgu_ref[rows, at : at + L] = dg
                    dgu_ref[rows, at + L : at + W] = du
                    weights[m // D, m % D : m % D + M, L * n : L * n + L] = (silu * up).astype(BF)
            low, high = (dotg(weights[i, :, :W], resident[D * i : D * i + D, :], TN) for i in range(2))
            out_ref[...] = (low + high).astype(BF)

        tiles = pl.BlockSpec((2, T, W), lambda j: (j, 0, 0))
        pipeline(body, (STEPS,), [block(W, D, row), tiles], [block(T, M, col), block(W, D, row)], hooks, full[2], gu0, dgu0, term[u])
        send_term(u)

    for u in (0, 1, 4, 5):
        mix_start(u)
    barrier((nx, ny, peer))
    for u in range(2):
        mix_wait(u)
        start_own(u)
    mix_wait(4)
    mix_wait(5)
    pipeline(norm_body, (T // W,), [block(W, D, row)], [block(W, D, row), block(D, W, col)], None, x, a0, a0t)
    in_a = load(a0, resident, 0)
    in_a.start()
    pass_on(0)
    start_own(2)
    pass_on_last(0)
    pass_on(1)
    start_own(3)
    arrived(0)
    in_a.wait()
    gate_up0(0)
    pass_on_last(1)
    pass_on(2)
    start_own(4)
    arrived(1)
    gate_up0(1)
    in_dy = load(dy, resident, 0)
    in_dy.start()
    pass_on_last(2)
    pass_on(3)
    start_own(5)
    arrived(2)
    pl.run_scoped(down_op, VMEM((FF, D), BF), pltpu.SemaphoreType.DMA)
    in_at = load(a1t, resident_t, 1)
    in_at.start()
    in_dy.wait()
    pass_on_last(3)
    pass_on(4)
    arrived(3)
    pipeline(dact_body, (STEPS,), [block(W, D, row)], [block(T, W, col)], None, full[3], dact1)
    in_a = load(a1, resident, 0)
    in_a.start()
    pass_on_last(4)
    in_at.wait()
    in_a.wait()
    arrived(4)
    gate_up1(0, {5: lambda: pass_on(5)})
    grad_gu(4, dgu1, None)
    pass_on_last(5)
    arrived(5)
    for u in range(6):
        for k in range(9):
            hop(u, k).wait_send()
    in_w = [load(full[4 + i], weights.at[i], 2 + i) for i in range(2)]
    for c in in_w:
        c.start()
    gate_up1(1, {4: fetch1(4), 6: pass1(4)})
    in_dy = load(dy, resident, 0)
    in_dy.start()
    grad_gu(5, dgu1, {1: fetch2(4), 4: pass2(4)})
    in_at = load(a0t, resident_t, 1)
    in_at.start()
    in_dy.wait()
    grad_down(3, act1, {4: fetch1(5), 6: pass1(5), 7: fetch3(4), 9: pass3(4)})
    for c in in_w:
        c.wait()
    grad_in(dgu1, h1, dy, dh1, True, {0: fetch2(5), 1: together(pass2(5), fetch1(3)), 3: pass1(3), 6: fetch3(5), 7: pass3(5)})
    act_back(2, {0: fetch2(3), 1: pass2(3), 6: fetch3(3), 7: pass3(3)})
    in_w = [load(full[i], weights.at[i], 2 + i) for i in range(2)]
    for c in in_w:
        c.start()
    in_at.wait()
    grad_gu(0, dgu0, {4: fetch1(2), 6: pass1(2)})
    grad_gu(1, dgu0, {1: fetch2(2), 3: pass2(2), 5: fetch1(0), 7: pass1(0)})
    for c in in_w:
        c.wait()
    grad_in(dgu0, x, dh1, dx, False, {1: fetch1(1), 2: together(pass1(1), fetch2(0)), 3: together(pass2(0), fetch3(2)), 4: pass3(2), 6: fetch2(1), 7: together(pass2(1), fetch3(0))})
    pass3(0)()
    fetch3(1)()
    pass3(1)()
    for u in (1, 2):
        for k in range(4, 8):
            copy(u, k).wait_send()
    for u in range(6):
        for k in range(4):
            copy(u, k).wait_send()


def solution(mesh):
    any_ = pl.BlockSpec(memory_space=ANY)
    dma = pltpu.SemaphoreType.DMA

    def s(*shape, dtype=BF):
        return jax.ShapeDtypeStruct(shape, dtype)

    outs = [s(2, GROWS, FF), s(2, GROWS, FF), s(2, DROWS, D), s(T, D)]
    outs += [s(*full_shape(u)) for u in range(6)] * 2
    outs += [s(4 * rows_of(u), full_shape(u)[1]) for u in range(6)]
    outs += [s(T, D), s(D, T), s(T, D), s(T, D), s(D, T), s(T, FF), s(2 * STEPS, T, W, dtype=F32), s(T, FF), s(T, 2 * FF), s(T, FF), s(T, D), s(T, 2 * FF)]
    scratch = [VMEM((2, D, FF), BF), VMEM((T, D), BF), VMEM((D, T), BF)]
    scratch += [VMEM((4, r, FF), BF) for r in (GROWS // 2, GROWS // 2, GROWS, GROWS)]
    scratch += [VMEM((2, r, D), BF) for r in (DROWS // 2, DROWS // 2, DROWS, DROWS)]
    scratch += [VMEM((3, GROWS, FF), BF), VMEM((3, DROWS, D), BF), VMEM((4, GROWS, FF), BF), VMEM((4, DROWS, D), BF)]
    scratch += [dma((6, 9)), dma((6, 9)), dma((6, 8)), dma((6, 8)), dma((6,)), dma((6,)), dma((4,)), dma((4,)), dma((2,))]
    step = pl.pallas_call(
        kernel,
        out_shape=outs,
        in_specs=[any_] * 4 + [pl.BlockSpec(memory_space=VMEM)],
        out_specs=[any_] * len(outs),
        scratch_shapes=scratch,
        compiler_params=pltpu.CompilerParams(collective_id=0, has_side_effects=True, vmem_limit_bytes=63 << 20),
        name="step",
    )

    def body(x, dy, wg, wu, wd):
        by_g, by_u, by_d, dx = step(x[0], dy[0], wg, wu, wd)[:4]
        return dx[None], by_g, by_u, by_d

    seq, rows = P(("rep", "dp"), None, None), P(None, "dp", None)
    out = P("rep", "dp", None)
    return jax.shard_map(body, mesh=mesh, in_specs=(seq, seq, rows, rows, rows), out_specs=(seq, out, out, out), check_vma=False)
```

```python
import jax
import jax.numpy as jnp
from jax import lax
from jax.experimental import pallas as pl
from jax.experimental.pallas import tpu as pltpu
from jax.sharding import PartitionSpec as P

BF, F32 = jnp.bfloat16, jnp.float32
T, D, FF = 2048, 1024, 2816
H = FF // 2
GROWS, DROWS = D // 8, FF // 8
UNITS = ((0, 0), (0, 1), (0, 2), (1, 2), (1, 0), (1, 1))
NT = (((1,), (1,)), ((), ()))
TN = (((0,), (0,)), ((), ()))
VMEM = pltpu.VMEM
ANY = pl.ANY
L, W, M = 128, 256, 512
STEPS = FF // W


def rows_of(u):
    return DROWS if UNITS[u][1] == 2 else GROWS


def full_shape(u):
    return (FF, D) if UNITS[u][1] == 2 else (D, FF)


def sigmoid(z):
    return 0.5 * jnp.tanh(0.5 * z) + 0.5


def dot(a, b):
    return jnp.dot(a, b, preferred_element_type=F32)


def dotg(a, b, dims):
    return lax.dot_general(a, b, dims, preferred_element_type=F32)


def places():
    me = lax.axis_index("dp")
    ix, iy, ic = me // 4, (me // 2) % 2, me % 2
    flip = lambda a, b, c: (ix + a - 2 * a * ix) * 4 + (iy + b - 2 * b * iy) * 2 + (ic + c - 2 * c * ic)
    return me, flip


def barrier(peers):
    sem = pltpu.get_barrier_semaphore()
    for p in peers:
        pl.semaphore_signal(sem, inc=1, device_id={"dp": p}, device_id_type=pl.DeviceIdType.MESH)
    pl.semaphore_wait(sem, len(peers))


def remote(src, dst, send, recv, to):
    return pltpu.make_async_remote_copy(src_ref=src, dst_ref=dst, send_sem=send, recv_sem=recv, device_id={"dp": to}, device_id_type=pl.DeviceIdType.MESH)


def block(rows, cols, index):
    return pl.BlockSpec((rows, cols), index)


def deep(rows, cols, index):
    return pl.BlockSpec((rows, cols), index, pipeline_mode=pl.Buffered(3))


def row(i):
    return i, 0


def col(j):
    return 0, j


def pipeline(body, grid, ins, outs, hooks, *arrays):
    def run(*refs):
        step = pl.program_id(0)
        if len(grid) == 2:
            step = step * grid[1] + pl.program_id(1)
        for at, work in (hooks or {}).items():
            pl.when(step == at)(work)
        body(*refs)

    pltpu.emit_pipeline(run, grid=grid, in_specs=ins, out_specs=outs)(*arrays)


def inverse_rms(wide):
    return lax.rsqrt(jnp.mean(wide * wide, -1, keepdims=True) + 1e-6)


def kernel(x, dy, wg, wu, wd, *refs):
    (by_g, by_u, by_d, dx), refs = refs[:4], refs[4:]
    full, term_gu, term_d, from_peer, refs = refs[:6], refs[6:8], refs[8:10], refs[10:16], refs[16:]
    a0, a0t, h1, a1, a1t, act0, gu0, act1, dgu1, dact1, dh1, dgu0, refs = *refs[:12], refs[12:]
    weights, resident, resident_t, *landings, gsend, dsend, gload, dload, gsem, gsem2, send, recv, local, mix, extra, lsem, osem = refs
    me, flip = places()
    nx, ny, peer, nxy = flip(1, 0, 0), flip(0, 1, 0), flip(0, 0, 1), flip(1, 1, 0)
    shards = [wd.at[n] if half == 2 else gload.at[2 * n + half] for n, half in UNITS]

    def load(src, dst, n):
        return pltpu.make_async_copy(src, dst, extra.at[n])

    def kind(u):
        return UNITS[u][1] == 2


    def part(u, b, half=None):
        r = rows_of(u)
        if half is None:
            return full[u].at[pl.ds(b * r, r), :]
        return full[u].at[pl.ds(b * r + half * (r // 2), r // 2), :]

    def piece(u):
        return 96 if kind(u) else 32

    def hop(u, k):
        r, p = rows_of(u), piece(u)
        low, high = pl.ds(0, p), pl.ds(p, r - p)
        mine = part(u, me)
        src, dst, to = (
            (shards[u].at[high, :], mine.at[high, :], nx),
            (shards[u].at[high, :], mine.at[high, :], ny),
            (shards[u], mine, peer),
            (part(u, nx, 0), part(u, nx, 0), ny),
            (part(u, ny, 1), part(u, ny, 1), nx),
            (part(u, nx), part(u, nx), peer),
            (part(u, ny), part(u, ny), peer),
            (part(u, nxy, 0), part(u, nxy, 0), peer),
            (part(u, nxy, 1), part(u, nxy, 1), peer),
            (shards[u].at[low, :], mine.at[low, :], nx),
            (shards[u].at[low, :], mine.at[low, :], ny),
        )[k]
        return remote(src, dst, gsem.at[u, k], gsem2.at[u, k], to)

    def own_copy(u):
        return pltpu.make_async_copy(shards[u], part(u, me), local.at[u])

    def start_first(u):
        hop(u, 9).start()
        hop(u, 10).start()

    def start_rest(u):
        for k in range(3):
            hop(u, k).start()
        own_copy(u).start()

    def pass_on(u):
        for k in (0, 1):
            hop(u, k + 9).wait_recv()
            hop(u, k).wait_recv()
            hop(u, k + 3).start()
            hop(u, k + 5).start()
        if u < 5:
            start_rest(u + 1)
        if u < 4:
            start_first(u + 2)

    def pass_on_last(u):
        for k in (3, 4):
            hop(u, k).wait_recv()
            hop(u, k + 4).start()

    def arrived(u):
        own_copy(u).wait()
        for k in (2, 5, 6, 7, 8):
            hop(u, k).wait_recv()

    def mix_start(u):
        n, half = UNITS[u]
        for j in range(STEPS):
            cols = pl.ds(half * H + L * j, L)
            for i, w in enumerate((wg, wu)):
                pltpu.make_async_copy(w.at[n, :, cols], shards[u].at[:, pl.ds(W * j + L * i, L)], mix.at[u]).start()

    def mix_wait(u):
        pltpu.make_async_copy(shards[u], shards[u], mix.at[u]).wait()

    where = (me, nx, ny, nxy)

    slot = (0, 1, 0, 1, 2, 3)
    before = {5: 4, 0: 5, 1: 0, 2: 3}

    def landing(u):
        return tuple(t.at[slot[u]] for t in landings[4 * kind(u) : 4 * kind(u) + 4])

    def sending(u):
        return dsend if kind(u) else gsend

    def loading(u):
        return dload if kind(u) else gload

    def term(u, b):
        n, half = UNITS[u]
        rows = pl.ds(b * rows_of(u), rows_of(u))
        return term_d[n].at[rows, :] if half == 2 else term_gu[n].at[rows, pl.ds(half * FF, FF)]

    def copy(u, k):
        r = rows_of(u)
        if k < 4:
            b = where[k]
            other = b + 1 - 2 * (b % 2)
            return remote(term(u, other), from_peer[u].at[pl.ds((b // 2) * r, r), :], send.at[u, k], recv.at[u, k], peer)
        s, (l1x, l1y, l2x, l2y) = sending(u), landing(u)
        half = r // 2
        src, dst, to = (
            (s.at[0, pl.ds(0, half), :], l1x, nx),
            (s.at[0, pl.ds(half, half), :], l1y, ny),
            (s.at[1], l2x, nx),
            (s.at[2], l2y, ny),
        )[k - 4]
        return remote(src, dst, send.at[u, k], recv.at[u, k], to)

    def send_term(u):
        for k in (3, 1, 2, 0):
            copy(u, k).start()

    def pairs(u, qs):
        r, v = rows_of(u), loading(u)
        for n, q in enumerate(qs):
            b = where[q]
            yield pltpu.make_async_copy(term(u, b), v.at[n], lsem.at[2 * n])
            yield pltpu.make_async_copy(from_peer[u].at[pl.ds((b // 2) * r, r), :], v.at[n + 2], lsem.at[2 * n + 1])

    def fetch(u, *qs):
        for q in qs:
            copy(u, q).wait_recv()
        for c in pairs(u, qs):
            c.start()

    def fetched(u, *qs):
        for c in pairs(u, qs):
            c.wait()

    def chunks(count, body):
        def step(i, _):
            body(pl.multiple_of(i * 16, 16))
            return 0

        lax.fori_loop(0, count // 16, step, 0)

    def both(v, n, rows):
        return v[n, rows, :].astype(F32) + v[n + 2, rows, :].astype(F32)

    def sent_before(u, *ks):
        if u in before:
            for k in ks:
                copy(before[u], k).wait_send()

    def fetch1(u):
        return lambda: fetch(u, 3)

    def fetch2(u):
        return lambda: fetch(u, 1, 2)

    def fetch3(u):
        return lambda: fetch(u, 0)

    def pass1(u):
        def work():
            fetched(u, 3)
            v, s = loading(u), sending(u)
            sent_before(u, 4, 5)

            def body(at):
                rows = pl.ds(at, 16)
                s[0, rows, :] = both(v, 0, rows).astype(BF)

            chunks(rows_of(u), body)
            copy(u, 4).start()
            copy(u, 5).start()

        return work

    def pass2(u):
        def work():
            fetched(u, 1, 2)
            v, s = loading(u), sending(u)
            l1x, l1y, _, _ = landing(u)
            sent_before(u, 6, 7)
            half = rows_of(u) // 2
            copy(u, 4).wait_recv()
            copy(u, 5).wait_recv()

            def body(at):
                low, high = pl.ds(at, 16), pl.ds(at + half, 16)
                s[1, low, :] = both(v, 0, low).astype(BF)
                s[1, high, :] = (both(v, 0, high) + l1y[low, :].astype(F32)).astype(BF)
                s[2, low, :] = (both(v, 1, low) + l1x[low, :].astype(F32)).astype(BF)
                s[2, high, :] = both(v, 1, high).astype(BF)

            chunks(half, body)
            copy(u, 6).start()
            copy(u, 7).start()

        return work

    def pass3(u):
        def work():
            fetched(u, 0)
            v = loading(u)
            _, _, l2x, l2y = landing(u)
            copy(u, 6).wait_recv()
            copy(u, 7).wait_recv()
            n, half = UNITS[u]

            def body(at):
                rows = pl.ds(at, 16)
                total = (both(v, 0, rows) + l2x[rows, :].astype(F32) + l2y[rows, :].astype(F32)).astype(BF)
                if kind(u):
                    v[1, rows, :] = total
                    return
                for j in range(STEPS):
                    for i in range(2):
                        v[1, rows, H * i + L * j : H * i + L * j + L] = total[:, W * j + L * i : W * j + L * i + L]

            chunks(rows_of(u), body)
            if kind(u):
                copies = [pltpu.make_async_copy(v.at[1], by_d.at[n], osem.at[0])]
            else:
                cols = pl.ds(half * H, H)
                copies = [pltpu.make_async_copy(v.at[1, :, pl.ds(H * i, H)], t.at[n, :, cols], osem.at[i]) for i, t in enumerate((by_g, by_u))]
            for c in copies:
                c.start()
            for c in copies:
                c.wait()

        return work

    def together(*works):
        def work():
            for w in works:
                w()

        return work


    def norm_into(wide, a_ref, at_ref):
        a = (wide * inverse_rms(wide)).astype(BF)
        a_ref[...] = a
        at_ref[...] = a.T

    def norm_body(x_ref, a_ref, at_ref):
        norm_into(x_ref[...].astype(F32), a_ref, at_ref)

    def gate_up0(half, hooks):
        def body(w_ref, gu_ref, act_ref):
            for m in range(0, T, M):
                s = dot(resident[m : m + M, :], w_ref[...])
                gu_ref[m : m + M, :] = s
                g, up = s[:, :L], s[:, L:]
                act_ref[m : m + M, :] = (g * sigmoid(g) * up).astype(BF)

        cols = lambda j: (0, j + STEPS * half)
        tiles = pl.BlockSpec((None, T, W), lambda j: (j + STEPS * half, 0, 0))
        pipeline(body, (STEPS,), [block(D, W, col)], [tiles, block(T, L, cols)], hooks, full[half], gu0, act0)

    def down_op(down, sem):
        in_down = pltpu.make_async_copy(full[2], down, sem)
        in_down.start()
        in_down.wait()

        def body(act_ref, x_ref, h_ref, a_ref, at_ref):
            h = x_ref[...] + dot(act_ref[...], down[...]).astype(BF)
            h_ref[...] = h
            norm_into(h.astype(F32), a_ref, at_ref)

        outs = [block(M, D, row), block(M, D, row), block(D, M, col)]
        pipeline(body, (T // M,), [block(M, FF, row), block(M, D, row)], outs, {2: lambda: pass_on(3)}, act0, x, h1, a1, a1t)

    def dact_body(w_ref, out_ref):
        for m in range(0, T, M):
            out_ref[m : m + M, :] = dotg(resident[m : m + M, :], w_ref[...], NT).astype(BF)

    def back(g, up, d):
        sg = sigmoid(g)
        silu = g * sg
        return silu, (d * up * (sg + silu * (1.0 - sg))).astype(BF), (d * silu).astype(BF)

    def gate_up1(half, hooks):
        def body(w_ref, dact_ref, act_ref, dgu_ref):
            for m in range(0, T, M):
                rows = slice(m, m + M)
                s = dot(resident[rows, :], w_ref[...])
                up = s[:, L:]
                silu, dg, du = back(s[:, :L], up, dact_ref[rows, :].astype(F32))
                act_ref[rows, :] = (silu * up).astype(BF)
                dgu_ref[rows, :L] = dg
                dgu_ref[rows, L:] = du

        cols = lambda j: (0, j + STEPS * half)
        ins, outs = [block(D, W, col), block(T, L, cols)], [block(T, L, cols), block(T, W, cols)]
        pipeline(body, (STEPS,), ins, outs, hooks, full[4 + half], dact1, act1, dgu1)

    def grad_gu(n, first, second, dgu, hooks):
        def body(d_ref, out_ref):
            for m in range(0, D, M):
                out_ref[m : m + M, :] = dot(resident_t[m : m + M, :], d_ref[...]).astype(BF)

        early = {7: together(*hooks.pop(7, ()), lambda: send_term(first))}
        pipeline(body, (STEPS,), [deep(T, M, col)], [block(D, M, col)], hooks | early, dgu, term_gu[n])
        send_term(second)

    def grad_down(u, act, hooks):
        def body(act_ref, out_ref):
            out_ref[...] = dotg(act_ref[...], resident[...], TN).astype(BF)

        pipeline(body, (STEPS,), [deep(T, W, col)], [block(W, D, row)], hooks, act, term_d[UNITS[u][0]])
        send_term(u)

    def grad_in(dgu, h, dh, out, keep, hooks):
        def body(d_ref, h_ref, dh_ref, out_ref):
            da = dotg(d_ref[:, :FF], weights[0], NT) + dotg(d_ref[:, FF:], weights[1], NT)
            d = da.astype(BF).astype(F32)
            wide = h_ref[...].astype(F32)
            scale = inverse_rms(wide)
            by_h = d * scale - wide * (scale * scale * scale * jnp.mean(d * wide, -1, keepdims=True))
            total = dh_ref[...] + by_h.astype(BF)
            out_ref[...] = total
            if keep:
                resident[pl.ds(pl.multiple_of(pl.program_id(0) * W, W), W), :] = total

        pipeline(body, (T // W,), [block(W, 2 * FF, row)] + [block(W, D, row)] * 2, [block(W, D, row)], hooks, dgu, h, dh, out)

    def act_back(u, hooks):
        def body(w_ref, gu_ref, dgu_ref, out_ref):
            for m in range(0, T, M):
                rows = slice(m, m + M)
                dd = dotg(resident[rows, :], w_ref[...], NT).astype(BF).astype(F32)
                for n in range(2):
                    at, up = W * n, gu_ref[n, rows, L:]
                    silu, dg, du = back(gu_ref[n, rows, :L], up, dd[:, L * n : L * n + L])
                    dgu_ref[rows, at : at + L] = dg
                    dgu_ref[rows, at + L : at + W] = du
                    weights[m // D, m % D : m % D + M, L * n : L * n + L] = (silu * up).astype(BF)
            low, high = (dotg(weights[i, :, :W], resident[D * i : D * i + D, :], TN) for i in range(2))
            out_ref[...] = (low + high).astype(BF)

        tiles = pl.BlockSpec((2, T, W), lambda j: (j, 0, 0))
        pipeline(body, (STEPS,), [block(W, D, row), tiles], [block(T, M, col), block(W, D, row)], hooks, full[2], gu0, dgu0, term_d[0])
        send_term(u)

    for u in (0, 1, 4, 5):
        mix_start(u)
    barrier((nx, ny, peer))
    mix_wait(0)
    start_first(0)
    start_rest(0)
    mix_wait(1)
    start_first(1)
    mix_wait(4)
    mix_wait(5)
    pipeline(norm_body, (T // W,), [block(W, D, row)], [block(W, D, row), block(D, W, col)], None, x, a0, a0t)
    in_a = load(a0, resident, 0)
    in_a.start()
    pass_on(0)
    pass_on_last(0)
    in_a.wait()
    arrived(0)
    gate_up0(0, {6: lambda: pass_on(1)})
    pass_on_last(1)
    arrived(1)
    gate_up0(1, {6: lambda: pass_on(2)})
    in_dy = load(dy, resident, 0)
    in_dy.start()
    pass_on_last(2)
    arrived(2)
    pl.run_scoped(down_op, VMEM((FF, D), BF), pltpu.SemaphoreType.DMA)
    in_at = load(a1t, resident_t, 1)
    in_at.start()
    in_dy.wait()
    pass_on_last(3)
    arrived(3)
    pipeline(dact_body, (STEPS,), [block(W, D, row)], [block(T, W, col)], {6: lambda: pass_on(4)}, full[3], dact1)
    in_a = load(a1, resident, 0)
    in_a.start()
    pass_on_last(4)
    in_at.wait()
    in_a.wait()
    arrived(4)
    gate_up1(0, {6: lambda: pass_on(5)})
    pass_on_last(5)
    arrived(5)
    in_w = [load(full[4 + i], weights.at[i], 2 + i) for i in range(2)]
    for c in in_w:
        c.start()
    gate_up1(1, None)
    for u in range(6):
        for k in range(11):
            hop(u, k).wait_send()
    in_dy = load(dy, resident, 0)
    in_dy.start()
    grad_gu(1, 4, 5, dgu1, {})
    in_at = load(a0t, resident_t, 1)
    in_at.start()
    in_dy.wait()
    grad_down(3, act1, {0: fetch1(4), 2: together(pass1(4), fetch1(5)), 5: pass1(5), 8: fetch2(4), 10: pass2(4)})
    for c in in_w:
        c.wait()
    grad_in(dgu1, h1, dy, dh1, True, {1: fetch2(5), 2: together(pass2(5), fetch1(3)), 3: pass1(3), 6: fetch3(4), 7: pass3(4)})
    act_back(2, {1: fetch3(5), 2: pass3(5), 3: fetch2(3), 4: pass2(3), 9: fetch3(3), 10: pass3(3)})
    in_w = [load(full[i], weights.at[i], 2 + i) for i in range(2)]
    for c in in_w:
        c.start()
    in_at.wait()
    grad_gu(0, 0, 1, dgu0, {2: fetch1(2), 3: pass1(2), 6: fetch2(2), 7: (pass2(2),), 10: fetch1(0)})
    for c in in_w:
        c.wait()
    grad_in(dgu0, x, dh1, dx, False, {0: pass1(0), 1: fetch1(1), 2: together(pass1(1), fetch2(0)), 3: together(pass2(0), fetch3(2)), 4: pass3(2), 5: fetch2(1), 6: pass2(1), 7: fetch3(0)})
    pass3(0)()
    fetch3(1)()
    pass3(1)()
    for u in (1, 2):
        for k in range(4, 8):
            copy(u, k).wait_send()
    for u in range(6):
        for k in range(4):
            copy(u, k).wait_send()


def hand_on_kernel(*refs):
    sources, targets, buffers, sems = refs[:4], refs[4:8], refs[8:12], refs[12]
    arrays = range(4)
    ins = [pltpu.make_async_copy(sources[i], buffers[i], sems.at[i]) for i in arrays]
    outs = [pltpu.make_async_copy(buffers[i], targets[i], sems.at[4 + i]) for i in arrays]
    for c in ins:
        c.start()
    for c, o in zip(ins, outs):
        c.wait()
        o.start()
    for o in outs:
        o.wait()


def solution(mesh):
    any_ = pl.BlockSpec(memory_space=ANY)
    dma = pltpu.SemaphoreType.DMA

    def s(*shape, dtype=BF):
        return jax.ShapeDtypeStruct(shape, dtype)

    outs = [s(2, GROWS, FF), s(2, GROWS, FF), s(2, DROWS, D), s(T, D)]
    outs += [s(*full_shape(u)) for u in range(6)]
    outs += [s(D, 2 * FF)] * 2 + [s(FF, D)] * 2
    outs += [s(4 * rows_of(u), full_shape(u)[1]) for u in range(6)]
    outs += [s(T, D), s(D, T), s(T, D), s(T, D), s(D, T), s(T, FF), s(2 * STEPS, T, W, dtype=F32), s(T, FF), s(T, 2 * FF), s(T, FF), s(T, D), s(T, 2 * FF)]
    scratch = [VMEM((2, D, FF), BF), VMEM((T, D), BF), VMEM((D, T), BF)]
    scratch += [VMEM((4, r, FF), BF) for r in (GROWS // 2, GROWS // 2, GROWS, GROWS)]
    scratch += [VMEM((2, r, D), BF) for r in (DROWS // 2, DROWS // 2, DROWS, DROWS)]
    scratch += [VMEM((3, GROWS, FF), BF), VMEM((3, DROWS, D), BF), VMEM((4, GROWS, FF), BF), VMEM((4, DROWS, D), BF)]
    scratch += [dma((6, 11)), dma((6, 11)), dma((6, 8)), dma((6, 8)), dma((6,)), dma((6,)), dma((4,)), dma((4,)), dma((2,))]
    step = pl.pallas_call(
        kernel,
        out_shape=outs,
        in_specs=[any_] * 4 + [pl.BlockSpec(memory_space=VMEM)],
        out_specs=[any_] * len(outs),
        scratch_shapes=scratch,
        compiler_params=pltpu.CompilerParams(collective_id=0, has_side_effects=True, vmem_limit_bytes=63 << 20),
        name="step",
    )

    hand_on = pl.pallas_call(
        hand_on_kernel,
        out_shape=outs[:4],
        in_specs=[any_] * 4,
        out_specs=[any_] * 4,
        scratch_shapes=[VMEM(o.shape, BF) for o in outs[:4]] + [dma((8,))],
        name="hand_on",
    )

    def body(x, dy, wg, wu, wd):
        by_g, by_u, by_d, dx = hand_on(*step(x[0], dy[0], wg, wu, wd)[:4])
        return dx[None], by_g, by_u, by_d

    seq, rows = P(("rep", "dp"), None, None), P(None, "dp", None)
    out = P("rep", "dp", None)
    return jax.shard_map(body, mesh=mesh, in_specs=(seq, seq, rows, rows, rows), out_specs=(seq, out, out, out), check_vma=False)
```

```python
import jax
import jax.numpy as jnp
from jax import lax
from jax.experimental import pallas as pl
from jax.experimental.pallas import tpu as pltpu
from jax.sharding import PartitionSpec as P

BF, F32 = jnp.bfloat16, jnp.float32
T, D, FF = 2048, 1024, 2816
H = FF // 2
GROWS, DROWS = D // 8, FF // 8
UNITS = ((0, 0), (0, 1), (0, 2), (1, 2), (1, 0), (1, 1))
NT = (((1,), (1,)), ((), ()))
TN = (((0,), (0,)), ((), ()))
VMEM = pltpu.VMEM
ANY = pl.ANY
L, W, M = 128, 256, 512
STEPS = FF // W


def rows_of(u):
    return DROWS if UNITS[u][1] == 2 else GROWS


def full_shape(u):
    return (FF, D) if UNITS[u][1] == 2 else (D, FF)


def sigmoid(z):
    return 0.5 * jnp.tanh(0.5 * z) + 0.5


def dot(a, b):
    return jnp.dot(a, b, preferred_element_type=F32)


def dotg(a, b, dims):
    return lax.dot_general(a, b, dims, preferred_element_type=F32)


def places():
    me = lax.axis_index("dp")
    ix, iy, ic = me // 4, (me // 2) % 2, me % 2
    flip = lambda a, b, c: (ix + a - 2 * a * ix) * 4 + (iy + b - 2 * b * iy) * 2 + (ic + c - 2 * c * ic)
    return me, flip


def barrier(peers):
    sem = pltpu.get_barrier_semaphore()
    for p in peers:
        pl.semaphore_signal(sem, inc=1, device_id={"dp": p}, device_id_type=pl.DeviceIdType.MESH)
    pl.semaphore_wait(sem, len(peers))


def remote(src, dst, send, recv, to):
    return pltpu.make_async_remote_copy(src_ref=src, dst_ref=dst, send_sem=send, recv_sem=recv, device_id={"dp": to}, device_id_type=pl.DeviceIdType.MESH)


def block(rows, cols, index):
    return pl.BlockSpec((rows, cols), index)


def deep(rows, cols, index):
    return pl.BlockSpec((rows, cols), index, pipeline_mode=pl.Buffered(3))


def row(i):
    return i, 0


def col(j):
    return 0, j


def pipeline(body, grid, ins, outs, hooks, *arrays):
    def run(*refs):
        step = pl.program_id(0)
        if len(grid) == 2:
            step = step * grid[1] + pl.program_id(1)
        for at, work in (hooks or {}).items():
            pl.when(step == at)(work)
        body(*refs)

    pltpu.emit_pipeline(run, grid=grid, in_specs=ins, out_specs=outs)(*arrays)


def inverse_rms(wide):
    return lax.rsqrt(jnp.mean(wide * wide, -1, keepdims=True) + 1e-6)


def kernel(x, dy, wg, wu, wd, *refs):
    (by_g, by_u, by_d, dx), refs = refs[:4], refs[4:]
    full, term_gu, term_d, from_peer, refs = refs[:6], refs[6:8], refs[8:10], refs[10:16], refs[16:]
    a0, a0t, h1, a1, a1t, act0, gu0, dgu1, dact1, dh1, dgu0, refs = *refs[:11], refs[11:]
    weights, resident, resident_t, *landings, gsend, dsend, gload, dload, gsem, gsem2, send, recv, local, mix, extra, lsem, osem = refs
    me, flip = places()
    nx, ny, peer, nxy = flip(1, 0, 0), flip(0, 1, 0), flip(0, 0, 1), flip(1, 1, 0)
    shards = [wd.at[n] if half == 2 else gload.at[2 * n + half] for n, half in UNITS]

    def load(src, dst, n):
        return pltpu.make_async_copy(src, dst, extra.at[n])

    def kind(u):
        return UNITS[u][1] == 2


    def part(u, b, half=None):
        r = rows_of(u)
        if half is None:
            return full[u].at[pl.ds(b * r, r), :]
        return full[u].at[pl.ds(b * r + half * (r // 2), r // 2), :]

    def piece(u):
        return 96 if kind(u) else 32

    def hop(u, k):
        r, p = rows_of(u), piece(u)
        low, high = pl.ds(0, p), pl.ds(p, r - p)
        mine = part(u, me)
        src, dst, to = (
            (shards[u].at[high, :], mine.at[high, :], nx),
            (shards[u].at[high, :], mine.at[high, :], ny),
            (shards[u], mine, peer),
            (part(u, nx, 0), part(u, nx, 0), ny),
            (part(u, ny, 1), part(u, ny, 1), nx),
            (part(u, nx), part(u, nx), peer),
            (part(u, ny), part(u, ny), peer),
            (part(u, nxy, 0), part(u, nxy, 0), peer),
            (part(u, nxy, 1), part(u, nxy, 1), peer),
            (shards[u].at[low, :], mine.at[low, :], nx),
            (shards[u].at[low, :], mine.at[low, :], ny),
        )[k]
        return remote(src, dst, gsem.at[u, k], gsem2.at[u, k], to)

    def own_copy(u):
        return pltpu.make_async_copy(shards[u], part(u, me), local.at[u])

    def start_first(u):
        hop(u, 9).start()
        hop(u, 10).start()

    def start_rest(u):
        for k in range(3):
            hop(u, k).start()
        own_copy(u).start()

    def pass_on(u):
        for k in (0, 1):
            hop(u, k + 9).wait_recv()
            hop(u, k).wait_recv()
            hop(u, k + 3).start()
            hop(u, k + 5).start()
        if u < 5:
            start_rest(u + 1)
        if u < 4:
            start_first(u + 2)

    def pass_on_last(u):
        for k in (3, 4):
            hop(u, k).wait_recv()
            hop(u, k + 4).start()

    def arrived(u):
        own_copy(u).wait()
        for k in (2, 5, 6, 7, 8):
            hop(u, k).wait_recv()

    def mix_start(u):
        n, half = UNITS[u]
        for j in range(STEPS):
            cols = pl.ds(half * H + L * j, L)
            for i, w in enumerate((wg, wu)):
                pltpu.make_async_copy(w.at[n, :, cols], shards[u].at[:, pl.ds(W * j + L * i, L)], mix.at[u]).start()

    def mix_wait(u):
        pltpu.make_async_copy(shards[u], shards[u], mix.at[u]).wait()

    where = (me, nx, ny, nxy)

    slot = (0, 1, 0, 1, 2, 3)
    before = {5: 4, 0: 5, 1: 0, 2: 3}

    def landing(u):
        return tuple(t.at[slot[u]] for t in landings[4 * kind(u) : 4 * kind(u) + 4])

    def sending(u):
        return dsend if kind(u) else gsend

    def loading(u):
        return dload if kind(u) else gload

    def term(u, b):
        n, half = UNITS[u]
        rows = pl.ds(b * rows_of(u), rows_of(u))
        return term_d[n].at[rows, :] if half == 2 else term_gu[n].at[rows, pl.ds(half * FF, FF)]

    def copy(u, k):
        r = rows_of(u)
        if k < 4:
            b = where[k]
            other = b + 1 - 2 * (b % 2)
            return remote(term(u, other), from_peer[u].at[pl.ds((b // 2) * r, r), :], send.at[u, k], recv.at[u, k], peer)
        s, (l1x, l1y, l2x, l2y) = sending(u), landing(u)
        half = r // 2
        src, dst, to = (
            (s.at[0, pl.ds(0, half), :], l1x, nx),
            (s.at[0, pl.ds(half, half), :], l1y, ny),
            (s.at[1], l2x, nx),
            (s.at[2], l2y, ny),
        )[k - 4]
        return remote(src, dst, send.at[u, k], recv.at[u, k], to)

    def send_term(u):
        for k in (3, 1, 2, 0):
            copy(u, k).start()

    def pairs(u, qs):
        r, v = rows_of(u), loading(u)
        for n, q in enumerate(qs):
            b = where[q]
            yield pltpu.make_async_copy(term(u, b), v.at[n], lsem.at[2 * n])
            yield pltpu.make_async_copy(from_peer[u].at[pl.ds((b // 2) * r, r), :], v.at[n + 2], lsem.at[2 * n + 1])

    def fetch(u, *qs):
        for q in qs:
            copy(u, q).wait_recv()
        for c in pairs(u, qs):
            c.start()

    def fetched(u, *qs):
        for c in pairs(u, qs):
            c.wait()

    def chunks(count, body):
        def step(i, _):
            body(pl.multiple_of(i * 16, 16))
            return 0

        lax.fori_loop(0, count // 16, step, 0)

    def both(v, n, rows):
        return v[n, rows, :].astype(F32) + v[n + 2, rows, :].astype(F32)

    def sent_before(u, *ks):
        if u in before:
            for k in ks:
                copy(before[u], k).wait_send()

    def fetch1(u):
        return lambda: fetch(u, 3)

    def fetch2(u):
        return lambda: fetch(u, 1, 2)

    def fetch3(u):
        return lambda: fetch(u, 0)

    def pass1(u):
        def work():
            fetched(u, 3)
            v, s = loading(u), sending(u)
            sent_before(u, 4, 5)

            def body(at):
                rows = pl.ds(at, 16)
                s[0, rows, :] = both(v, 0, rows).astype(BF)

            chunks(rows_of(u), body)
            copy(u, 4).start()
            copy(u, 5).start()

        return work

    def pass2(u):
        def work():
            fetched(u, 1, 2)
            v, s = loading(u), sending(u)
            l1x, l1y, _, _ = landing(u)
            sent_before(u, 6, 7)
            half = rows_of(u) // 2
            copy(u, 4).wait_recv()
            copy(u, 5).wait_recv()

            def body(at):
                low, high = pl.ds(at, 16), pl.ds(at + half, 16)
                s[1, low, :] = both(v, 0, low).astype(BF)
                s[1, high, :] = (both(v, 0, high) + l1y[low, :].astype(F32)).astype(BF)
                s[2, low, :] = (both(v, 1, low) + l1x[low, :].astype(F32)).astype(BF)
                s[2, high, :] = both(v, 1, high).astype(BF)

            chunks(half, body)
            copy(u, 6).start()
            copy(u, 7).start()

        return work

    def pass3(u):
        def work():
            fetched(u, 0)
            v = loading(u)
            _, _, l2x, l2y = landing(u)
            copy(u, 6).wait_recv()
            copy(u, 7).wait_recv()
            n, half = UNITS[u]

            def body(at):
                rows = pl.ds(at, 16)
                total = (both(v, 0, rows) + l2x[rows, :].astype(F32) + l2y[rows, :].astype(F32)).astype(BF)
                if kind(u):
                    v[1, rows, :] = total
                    return
                for j in range(STEPS):
                    for i in range(2):
                        v[1, rows, H * i + L * j : H * i + L * j + L] = total[:, W * j + L * i : W * j + L * i + L]

            chunks(rows_of(u), body)
            if kind(u):
                copies = [pltpu.make_async_copy(v.at[1], by_d.at[n], osem.at[0])]
            else:
                cols = pl.ds(half * H, H)
                copies = [pltpu.make_async_copy(v.at[1, :, pl.ds(H * i, H)], t.at[n, :, cols], osem.at[i]) for i, t in enumerate((by_g, by_u))]
            for c in copies:
                c.start()
            for c in copies:
                c.wait()

        return work

    def together(*works):
        def work():
            for w in works:
                w()

        return work


    def norm_into(wide, a_ref, at_ref):
        a = (wide * inverse_rms(wide)).astype(BF)
        a_ref[...] = a
        at_ref[...] = a.T

    def norm_body(x_ref, a_ref, at_ref):
        norm_into(x_ref[...].astype(F32), a_ref, at_ref)

    def gate_up0(half, hooks):
        def body(w_ref, gu_ref, act_ref):
            for m in range(0, T, M):
                s = dot(resident[m : m + M, :], w_ref[...])
                gu_ref[m : m + M, :] = s
                g, up = s[:, :L], s[:, L:]
                act_ref[m : m + M, :] = (g * sigmoid(g) * up).astype(BF)

        cols = lambda j: (0, j + STEPS * half)
        tiles = pl.BlockSpec((None, T, W), lambda j: (j + STEPS * half, 0, 0))
        pipeline(body, (STEPS,), [block(D, W, col)], [tiles, block(T, L, cols)], hooks, full[half], gu0, act0)

    def down_op(down, sem):
        in_down = pltpu.make_async_copy(full[2], down, sem)
        in_down.start()
        in_down.wait()

        def body(act_ref, x_ref, h_ref, a_ref, at_ref):
            h = x_ref[...] + dot(act_ref[...], down[...]).astype(BF)
            h_ref[...] = h
            norm_into(h.astype(F32), a_ref, at_ref)

        outs = [block(M, D, row), block(M, D, row), block(D, M, col)]
        pipeline(body, (T // M,), [block(M, FF, row), block(M, D, row)], outs, {2: lambda: pass_on(3)}, act0, x, h1, a1, a1t)

    def dact_body(w_ref, out_ref):
        for m in range(0, T, M):
            out_ref[m : m + M, :] = dotg(resident[m : m + M, :], w_ref[...], NT).astype(BF)

    def back(g, up, d):
        sg = sigmoid(g)
        silu = g * sg
        return silu, (d * up * (sg + silu * (1.0 - sg))).astype(BF), (d * silu).astype(BF)

    def gate_up1(half, hooks):
        def body(w_ref, dact_ref, dgu_ref, out_ref):
            for m in range(0, T, M):
                rows = slice(m, m + M)
                s = dot(resident[rows, :], w_ref[...])
                up = s[:, L:]
                silu, dg, du = back(s[:, :L], up, dact_ref[rows, :].astype(F32))
                weights[m // D, m % D : m % D + M, D : D + L] = (silu * up).astype(BF)
                dgu_ref[rows, :L] = dg
                dgu_ref[rows, L:] = du
            low, high = (dotg(weights[i, :, D : D + L], weights[i, :, :D], TN) for i in range(2))
            out_ref[...] = (low + high).astype(BF)

        cols = lambda j: (0, j + STEPS * half)
        ins, outs = [block(D, W, col), block(T, L, cols)], [block(T, W, cols), block(L, D, lambda j: (j + STEPS * half, 0))]
        pipeline(body, (STEPS,), ins, outs, hooks, full[4 + half], dact1, dgu1, term_d[1])

    def grad_gu(n, first, second, dgu, hooks):
        def body(d_ref, out_ref):
            for m in range(0, D, M):
                out_ref[m : m + M, :] = dot(resident_t[m : m + M, :], d_ref[...]).astype(BF)

        early = {7: together(*hooks.pop(7, ()), lambda: send_term(first))}
        pipeline(body, (STEPS,), [deep(T, M, col)], [block(D, M, col)], hooks | early, dgu, term_gu[n])
        send_term(second)

    def grad_in(dgu, h, dh, out, keep, hooks):
        def body(d_ref, h_ref, dh_ref, out_ref):
            da = dotg(d_ref[:, :FF], weights[0], NT) + dotg(d_ref[:, FF:], weights[1], NT)
            d = da.astype(BF).astype(F32)
            wide = h_ref[...].astype(F32)
            scale = inverse_rms(wide)
            by_h = d * scale - wide * (scale * scale * scale * jnp.mean(d * wide, -1, keepdims=True))
            total = dh_ref[...] + by_h.astype(BF)
            out_ref[...] = total
            if keep:
                resident[pl.ds(pl.multiple_of(pl.program_id(0) * W, W), W), :] = total

        pipeline(body, (T // W,), [block(W, 2 * FF, row)] + [block(W, D, row)] * 2, [block(W, D, row)], hooks, dgu, h, dh, out)

    def act_back(u, hooks):
        def body(w_ref, gu_ref, dgu_ref, out_ref):
            for m in range(0, T, W):
                rows = slice(m, m + W)
                dd = dotg(resident[rows, :], w_ref[...], NT).astype(BF).astype(F32)
                for n in range(2):
                    at, up = W * n, gu_ref[n, rows, L:]
                    silu, dg, du = back(gu_ref[n, rows, :L], up, dd[:, L * n : L * n + L])
                    dgu_ref[rows, at : at + L] = dg
                    dgu_ref[rows, at + L : at + W] = du
                    weights[m // D, m % D : m % D + W, L * n : L * n + L] = (silu * up).astype(BF)
            low, high = (dotg(weights[i, :, :W], resident[D * i : D * i + D, :], TN) for i in range(2))
            out_ref[...] = (low + high).astype(BF)

        tiles = pl.BlockSpec((2, T, W), lambda j: (j, 0, 0))
        pipeline(body, (STEPS,), [block(W, D, row), tiles], [block(T, M, col), block(W, D, row)], hooks, full[2], gu0, dgu0, term_d[0])
        send_term(u)

    for u in (0, 1, 4, 5):
        mix_start(u)
    barrier((nx, ny, peer))
    mix_wait(0)
    start_first(0)
    start_rest(0)
    mix_wait(1)
    start_first(1)
    mix_wait(4)
    mix_wait(5)
    pipeline(norm_body, (T // W,), [block(W, D, row)], [block(W, D, row), block(D, W, col)], None, x, a0, a0t)
    in_a = load(a0, resident, 0)
    in_a.start()
    pass_on(0)
    pass_on_last(0)
    in_a.wait()
    arrived(0)
    gate_up0(0, {6: lambda: pass_on(1)})
    pass_on_last(1)
    arrived(1)
    gate_up0(1, {6: lambda: pass_on(2)})
    in_dy = load(dy, resident, 0)
    in_dy.start()
    pass_on_last(2)
    arrived(2)
    pl.run_scoped(down_op, VMEM((FF, D), BF), pltpu.SemaphoreType.DMA)
    in_at = load(a1t, resident_t, 1)
    in_at.start()
    in_dy.wait()
    pass_on_last(3)
    arrived(3)
    pipeline(dact_body, (STEPS,), [block(W, D, row)], [block(T, W, col)], {6: lambda: pass_on(4)}, full[3], dact1)
    in_a = load(a1, resident, 0)
    in_a.start()
    in_dy = [load(dy.at[pl.ds(D * i, D), :], weights.at[i, :, pl.ds(0, D)], 2 + i) for i in range(2)]
    for c in in_dy:
        c.start()
    pass_on_last(4)
    in_at.wait()
    in_a.wait()
    for c in in_dy:
        c.wait()
    arrived(4)
    gate_up1(0, {6: lambda: pass_on(5)})
    pass_on_last(5)
    arrived(5)
    gate_up1(1, None)
    send_term(3)
    in_w = [load(full[4 + i], weights.at[i], 2 + i) for i in range(2)]
    for c in in_w:
        c.start()
    for u in range(6):
        for k in range(11):
            hop(u, k).wait_send()
    grad_gu(1, 4, 5, dgu1, {3: fetch1(3), 4: pass1(3), 8: fetch2(3), 9: pass2(3)})
    in_at = load(a0t, resident_t, 1)
    in_at.start()
    for c in in_w:
        c.wait()
    grad_in(dgu1, h1, dy, dh1, True, {0: fetch1(4), 1: together(pass1(4), fetch1(5)), 2: pass1(5), 3: fetch2(4), 4: together(pass2(4), fetch3(3)), 5: together(pass3(3), fetch2(5)), 6: pass2(5)})
    act_back(2, {3: fetch3(4), 4: pass3(4), 8: fetch3(5), 9: pass3(5)})
    in_w = [load(full[i], weights.at[i], 2 + i) for i in range(2)]
    for c in in_w:
        c.start()
    in_at.wait()
    grad_gu(0, 0, 1, dgu0, {2: fetch1(2), 3: pass1(2), 6: fetch2(2), 7: (pass2(2),), 10: fetch1(0)})
    for c in in_w:
        c.wait()
    grad_in(dgu0, x, dh1, dx, False, {0: pass1(0), 1: fetch1(1), 2: together(pass1(1), fetch2(0)), 3: together(pass2(0), fetch3(2)), 4: pass3(2), 5: fetch2(1), 6: pass2(1), 7: fetch3(0)})
    pass3(0)()
    fetch3(1)()
    pass3(1)()
    for u in (1, 2):
        for k in range(4, 8):
            copy(u, k).wait_send()
    for u in range(6):
        for k in range(4):
            copy(u, k).wait_send()


def hand_on_kernel(*refs):
    sources, targets, buffers, sems = refs[:4], refs[4:8], refs[8:12], refs[12]
    arrays = range(4)
    ins = [pltpu.make_async_copy(sources[i], buffers[i], sems.at[i]) for i in arrays]
    outs = [pltpu.make_async_copy(buffers[i], targets[i], sems.at[4 + i]) for i in arrays]
    for c in ins:
        c.start()
    for c, o in zip(ins, outs):
        c.wait()
        o.start()
    for o in outs:
        o.wait()


def solution(mesh):
    any_ = pl.BlockSpec(memory_space=ANY)
    dma = pltpu.SemaphoreType.DMA

    def s(*shape, dtype=BF):
        return jax.ShapeDtypeStruct(shape, dtype)

    outs = [s(2, GROWS, FF), s(2, GROWS, FF), s(2, DROWS, D), s(T, D)]
    outs += [s(*full_shape(u)) for u in range(6)]
    outs += [s(D, 2 * FF)] * 2 + [s(FF, D)] * 2
    outs += [s(4 * rows_of(u), full_shape(u)[1]) for u in range(6)]
    outs += [s(T, D), s(D, T), s(T, D), s(T, D), s(D, T), s(T, FF), s(2 * STEPS, T, W, dtype=F32), s(T, 2 * FF), s(T, FF), s(T, D), s(T, 2 * FF)]
    scratch = [VMEM((2, D, FF), BF), VMEM((T, D), BF), VMEM((D, T), BF)]
    scratch += [VMEM((4, r, FF), BF) for r in (GROWS // 2, GROWS // 2, GROWS, GROWS)]
    scratch += [VMEM((2, r, D), BF) for r in (DROWS // 2, DROWS // 2, DROWS, DROWS)]
    scratch += [VMEM((3, GROWS, FF), BF), VMEM((3, DROWS, D), BF), VMEM((4, GROWS, FF), BF), VMEM((4, DROWS, D), BF)]
    scratch += [dma((6, 11)), dma((6, 11)), dma((6, 8)), dma((6, 8)), dma((6,)), dma((6,)), dma((4,)), dma((4,)), dma((2,))]
    step = pl.pallas_call(
        kernel,
        out_shape=outs,
        in_specs=[any_] * 4 + [pl.BlockSpec(memory_space=VMEM)],
        out_specs=[any_] * len(outs),
        scratch_shapes=scratch,
        compiler_params=pltpu.CompilerParams(collective_id=0, has_side_effects=True, vmem_limit_bytes=63 << 20),
        name="step",
    )

    hand_on = pl.pallas_call(
        hand_on_kernel,
        out_shape=outs[:4],
        in_specs=[any_] * 4,
        out_specs=[any_] * 4,
        scratch_shapes=[VMEM(o.shape, BF) for o in outs[:4]] + [dma((8,))],
        name="hand_on",
    )

    def body(x, dy, wg, wu, wd):
        by_g, by_u, by_d, dx = hand_on(*step(x[0], dy[0], wg, wu, wd)[:4])
        return dx[None], by_g, by_u, by_d

    seq, rows = P(("rep", "dp"), None, None), P(None, "dp", None)
    out = P("rep", "dp", None)
    return jax.shard_map(body, mesh=mesh, in_specs=(seq, seq, rows, rows, rows), out_specs=(seq, out, out, out), check_vma=False)
```

```python
import jax
import jax.numpy as jnp
from jax import lax
from jax.experimental import pallas as pl
from jax.experimental.pallas import tpu as pltpu
from jax.sharding import PartitionSpec as P

BF, F32 = jnp.bfloat16, jnp.float32
T, D, FF = 2048, 1024, 2816
H = FF // 2
GROWS, DROWS = D // 8, FF // 8
UNITS = ((0, 0), (0, 1), (0, 2), (1, 2), (1, 0), (1, 1))
NT = (((1,), (1,)), ((), ()))
TN = (((0,), (0,)), ((), ()))
VMEM = pltpu.VMEM
ANY = pl.ANY
L, W, M = 128, 256, 512
STEPS = FF // W


def rows_of(u):
    return DROWS if UNITS[u][1] == 2 else GROWS


def full_shape(u):
    return (FF, D) if UNITS[u][1] == 2 else (D, FF)


def sigmoid(z):
    return 0.5 * jnp.tanh(0.5 * z) + 0.5


def dot(a, b):
    return jnp.dot(a, b, preferred_element_type=F32)


def dotg(a, b, dims):
    return lax.dot_general(a, b, dims, preferred_element_type=F32)


def places():
    me = lax.axis_index("dp")
    ix, iy, ic = me // 4, (me // 2) % 2, me % 2
    flip = lambda a, b, c: (ix + a - 2 * a * ix) * 4 + (iy + b - 2 * b * iy) * 2 + (ic + c - 2 * c * ic)
    return me, flip


def barrier(peers):
    sem = pltpu.get_barrier_semaphore()
    for p in peers:
        pl.semaphore_signal(sem, inc=1, device_id={"dp": p}, device_id_type=pl.DeviceIdType.MESH)
    pl.semaphore_wait(sem, len(peers))


def remote(src, dst, send, recv, to):
    return pltpu.make_async_remote_copy(src_ref=src, dst_ref=dst, send_sem=send, recv_sem=recv, device_id={"dp": to}, device_id_type=pl.DeviceIdType.MESH)


def block(rows, cols, index):
    return pl.BlockSpec((rows, cols), index)


def deep(rows, cols, index):
    return pl.BlockSpec((rows, cols), index, pipeline_mode=pl.Buffered(3))


def row(i):
    return i, 0


def col(j):
    return 0, j


def pipeline(body, grid, ins, outs, hooks, *arrays):
    def run(*refs):
        step = pl.program_id(0)
        if len(grid) == 2:
            step = step * grid[1] + pl.program_id(1)
        for at, work in (hooks or {}).items():
            pl.when(step == at)(work)
        body(*refs)

    pltpu.emit_pipeline(run, grid=grid, in_specs=ins, out_specs=outs)(*arrays)


def inverse_rms(wide):
    return lax.rsqrt(jnp.mean(wide * wide, -1, keepdims=True) + 1e-6)


def kernel(x, dy, wg, wu, wd, *refs):
    (by_g, by_u, by_d, dx), refs = refs[:4], refs[4:]
    full, term_gu, term_d, from_peer, refs = refs[:6], refs[6:8], refs[8:10], refs[10:16], refs[16:]
    a0, a0t, h1, a1, a1t, act0, gu0, dgu1, dact1, dh1, dgu0, refs = *refs[:11], refs[11:]
    weights, resident, resident_t, *landings, gsend, dsend, gload, dload, gsem, gsem2, send, recv, local, mix, extra, lsem, osem = refs
    me, flip = places()
    nx, ny, peer, nxy = flip(1, 0, 0), flip(0, 1, 0), flip(0, 0, 1), flip(1, 1, 0)
    shards = [wd.at[n] if half == 2 else gload.at[2 * n + half] for n, half in UNITS]

    def load(src, dst, n):
        return pltpu.make_async_copy(src, dst, extra.at[n])

    def kind(u):
        return UNITS[u][1] == 2


    def part(u, b, half=None):
        r = rows_of(u)
        if half is None:
            return full[u].at[pl.ds(b * r, r), :]
        return full[u].at[pl.ds(b * r + half * (r // 2), r // 2), :]

    def piece(u):
        return 96 if kind(u) else 32

    def hop(u, k):
        r, p = rows_of(u), piece(u)
        low, high = pl.ds(0, p), pl.ds(p, r - p)
        mine = part(u, me)
        src, dst, to = (
            (shards[u].at[high, :], mine.at[high, :], nx),
            (shards[u].at[high, :], mine.at[high, :], ny),
            (shards[u], mine, peer),
            (part(u, nx, 0), part(u, nx, 0), ny),
            (part(u, ny, 1), part(u, ny, 1), nx),
            (part(u, nx), part(u, nx), peer),
            (part(u, ny), part(u, ny), peer),
            (part(u, nxy, 0), part(u, nxy, 0), peer),
            (part(u, nxy, 1), part(u, nxy, 1), peer),
            (shards[u].at[low, :], mine.at[low, :], nx),
            (shards[u].at[low, :], mine.at[low, :], ny),
        )[k]
        return remote(src, dst, gsem.at[u, k], gsem2.at[u, k], to)

    def own_copy(u):
        return pltpu.make_async_copy(shards[u], part(u, me), local.at[u])

    def start_first(u):
        hop(u, 9).start()
        hop(u, 10).start()

    def start_rest(u):
        for k in range(3):
            hop(u, k).start()
        own_copy(u).start()

    def pass_on(u):
        for k in (0, 1):
            hop(u, k + 9).wait_recv()
            hop(u, k).wait_recv()
            hop(u, k + 3).start()
            hop(u, k + 5).start()
        if u < 5:
            start_rest(u + 1)
        if u < 4:
            start_first(u + 2)

    def pass_on_last(u):
        for k in (3, 4):
            hop(u, k).wait_recv()
            hop(u, k + 4).start()

    def arrived(u):
        own_copy(u).wait()
        for k in (2, 5, 6, 7, 8):
            hop(u, k).wait_recv()

    def mix_start(u):
        n, half = UNITS[u]
        for j in range(STEPS):
            cols = pl.ds(half * H + L * j, L)
            for i, w in enumerate((wg, wu)):
                pltpu.make_async_copy(w.at[n, :, cols], shards[u].at[:, pl.ds(W * j + L * i, L)], mix.at[u]).start()

    def mix_wait(u):
        pltpu.make_async_copy(shards[u], shards[u], mix.at[u]).wait()

    where = (me, nx, ny, nxy)

    slot = (0, 1, 0, 1, 2, 3)
    before = {5: 4, 0: 5, 1: 0, 2: 3}

    def landing(u):
        return tuple(t.at[slot[u]] for t in landings[4 * kind(u) : 4 * kind(u) + 4])

    def sending(u):
        return dsend if kind(u) else gsend

    def loading(u):
        return dload if kind(u) else gload

    def term(u, b):
        n, half = UNITS[u]
        rows = pl.ds(b * rows_of(u), rows_of(u))
        return term_d[n].at[rows, :] if half == 2 else term_gu[n].at[rows, pl.ds(half * FF, FF)]

    def copy(u, k):
        r = rows_of(u)
        if k < 4:
            b = where[k]
            other = b + 1 - 2 * (b % 2)
            return remote(term(u, other), from_peer[u].at[pl.ds((b // 2) * r, r), :], send.at[u, k], recv.at[u, k], peer)
        s, (l1x, l1y, l2x, l2y) = sending(u), landing(u)
        half = r // 2
        src, dst, to = (
            (s.at[0, pl.ds(0, half), :], l1x, nx),
            (s.at[0, pl.ds(half, half), :], l1y, ny),
            (s.at[1], l2x, nx),
            (s.at[2], l2y, ny),
        )[k - 4]
        return remote(src, dst, send.at[u, k], recv.at[u, k], to)

    def send_term(u):
        for k in (3, 1, 2, 0):
            copy(u, k).start()

    def pairs(u, qs):
        r, v = rows_of(u), loading(u)
        for n, q in enumerate(qs):
            b = where[q]
            yield pltpu.make_async_copy(term(u, b), v.at[n], lsem.at[2 * n])
            yield pltpu.make_async_copy(from_peer[u].at[pl.ds((b // 2) * r, r), :], v.at[n + 2], lsem.at[2 * n + 1])

    def fetch(u, *qs):
        for q in qs:
            copy(u, q).wait_recv()
        for c in pairs(u, qs):
            c.start()

    def fetched(u, *qs):
        for c in pairs(u, qs):
            c.wait()

    def chunks(count, body):
        def step(i, _):
            body(pl.multiple_of(i * 16, 16))
            return 0

        lax.fori_loop(0, count // 16, step, 0)

    def both(v, n, rows):
        return v[n, rows, :].astype(F32) + v[n + 2, rows, :].astype(F32)

    def sent_before(u, *ks):
        if u in before:
            for k in ks:
                copy(before[u], k).wait_send()

    def fetch1(u):
        return lambda: fetch(u, 3)

    def fetch2(u):
        return lambda: fetch(u, 1, 2)

    def fetch3(u):
        return lambda: fetch(u, 0)

    def pass1(u):
        def work():
            fetched(u, 3)
            v, s = loading(u), sending(u)
            sent_before(u, 4, 5)

            def body(at):
                rows = pl.ds(at, 16)
                s[0, rows, :] = both(v, 0, rows).astype(BF)

            chunks(rows_of(u), body)
            copy(u, 4).start()
            copy(u, 5).start()

        return work

    def pass2(u):
        def work():
            fetched(u, 1, 2)
            v, s = loading(u), sending(u)
            l1x, l1y, _, _ = landing(u)
            sent_before(u, 6, 7)
            half = rows_of(u) // 2
            copy(u, 4).wait_recv()
            copy(u, 5).wait_recv()

            def body(at):
                low, high = pl.ds(at, 16), pl.ds(at + half, 16)
                s[1, low, :] = both(v, 0, low).astype(BF)
                s[1, high, :] = (both(v, 0, high) + l1y[low, :].astype(F32)).astype(BF)
                s[2, low, :] = (both(v, 1, low) + l1x[low, :].astype(F32)).astype(BF)
                s[2, high, :] = both(v, 1, high).astype(BF)

            chunks(half, body)
            copy(u, 6).start()
            copy(u, 7).start()

        return work

    def pass3(u):
        def work():
            fetched(u, 0)
            v = loading(u)
            _, _, l2x, l2y = landing(u)
            copy(u, 6).wait_recv()
            copy(u, 7).wait_recv()
            n, half = UNITS[u]

            def body(at):
                rows = pl.ds(at, 16)
                total = (both(v, 0, rows) + l2x[rows, :].astype(F32) + l2y[rows, :].astype(F32)).astype(BF)
                if kind(u):
                    v[1, rows, :] = total
                    return
                for j in range(STEPS):
                    for i in range(2):
                        v[1, rows, H * i + L * j : H * i + L * j + L] = total[:, W * j + L * i : W * j + L * i + L]

            chunks(rows_of(u), body)
            if kind(u):
                copies = [pltpu.make_async_copy(v.at[1], by_d.at[n], osem.at[0])]
            else:
                cols = pl.ds(half * H, H)
                copies = [pltpu.make_async_copy(v.at[1, :, pl.ds(H * i, H)], t.at[n, :, cols], osem.at[i]) for i, t in enumerate((by_g, by_u))]
            for c in copies:
                c.start()
            for c in copies:
                c.wait()

        return work

    def together(*works):
        def work():
            for w in works:
                w()

        return work


    def norm_into(wide, a_ref, at_ref):
        a = (wide * inverse_rms(wide)).astype(BF)
        a_ref[...] = a
        at_ref[...] = a.T

    def norm_body(x_ref, a_ref, at_ref):
        norm_into(x_ref[...].astype(F32), a_ref, at_ref)

    def gate_up0(half, hooks):
        def body(w_ref, gu_ref, act_ref):
            for m in range(0, T, M):
                s = dot(resident[m : m + M, :], w_ref[...])
                gu_ref[m : m + M, :] = s
                g, up = s[:, :L], s[:, L:]
                act_ref[m : m + M, :] = (g * sigmoid(g) * up).astype(BF)

        cols = lambda j: (0, j + STEPS * half)
        tiles = pl.BlockSpec((None, T, W), lambda j: (j + STEPS * half, 0, 0))
        pipeline(body, (STEPS,), [block(D, W, col)], [tiles, block(T, L, cols)], hooks, full[half], gu0, act0)

    def down_op(down, sem):
        in_down = pltpu.make_async_copy(full[2], down, sem)
        in_down.start()
        in_down.wait()

        def body(act_ref, x_ref, h_ref, a_ref, at_ref):
            h = x_ref[...] + dot(act_ref[...], down[...]).astype(BF)
            h_ref[...] = h
            norm_into(h.astype(F32), a_ref, at_ref)

        outs = [block(M, D, row), block(M, D, row), block(D, M, col)]
        pipeline(body, (T // M,), [block(M, FF, row), block(M, D, row)], outs, {2: lambda: pass_on(3)}, act0, x, h1, a1, a1t)

    def dact_body(w_ref, out_ref):
        for m in range(0, T, M):
            out_ref[m : m + M, :] = dotg(resident[m : m + M, :], w_ref[...], NT).astype(BF)

    def back(g, up, d):
        sg = sigmoid(g)
        silu = g * sg
        return silu, (d * up * (sg + silu * (1.0 - sg))).astype(BF), (d * silu).astype(BF)

    def gate_up1(half, hooks):
        def body(w_ref, dact_ref, dgu_ref, out_ref):
            for m in range(0, T, M):
                rows = slice(m, m + M)
                s = dot(resident[rows, :], w_ref[...])
                up = s[:, L:]
                silu, dg, du = back(s[:, :L], up, dact_ref[rows, :].astype(F32))
                weights[m // D, m % D : m % D + M, D : D + L] = (silu * up).astype(BF)
                dgu_ref[rows, :L] = dg
                dgu_ref[rows, L:] = du
            low, high = (dotg(weights[i, :, D : D + L], weights[i, :, :D], TN) for i in range(2))
            out_ref[...] = (low + high).astype(BF)

        cols = lambda j: (0, j + STEPS * half)
        ins, outs = [block(D, W, col), block(T, L, cols)], [block(T, W, cols), block(L, D, lambda j: (j + STEPS * half, 0))]
        pipeline(body, (STEPS,), ins, outs, hooks, full[4 + half], dact1, dgu1, term_d[1])

    def grad_gu(n, first, second, dgu, hooks):
        def body(d_ref, out_ref):
            for m in range(0, D, M):
                out_ref[m : m + M, :] = dot(resident_t[m : m + M, :], d_ref[...]).astype(BF)

        early = {7: together(*hooks.pop(7, ()), lambda: send_term(first))}
        pipeline(body, (STEPS,), [deep(T, M, col)], [block(D, M, col)], hooks | early, dgu, term_gu[n])
        send_term(second)

    def grad_in(dgu, h, dh, out, keep, hooks):
        def body(d_ref, h_ref, dh_ref, out_ref):
            da = dotg(d_ref[:, :FF], weights[0], NT) + dotg(d_ref[:, FF:], weights[1], NT)
            d = da.astype(BF).astype(F32)
            wide = h_ref[...].astype(F32)
            scale = inverse_rms(wide)
            by_h = d * scale - wide * (scale * scale * scale * jnp.mean(d * wide, -1, keepdims=True))
            total = dh_ref[...] + by_h.astype(BF)
            out_ref[...] = total
            if keep:
                resident[pl.ds(pl.multiple_of(pl.program_id(0) * W, W), W), :] = total

        pipeline(body, (T // W,), [block(W, 2 * FF, row)] + [block(W, D, row)] * 2, [block(W, D, row)], hooks, dgu, h, dh, out)

    def act_back(u, hooks):
        def body(w_ref, gu_ref, dgu_ref, out_ref):
            for m in range(0, T, W):
                rows = slice(m, m + W)
                dd = dotg(resident[rows, :], w_ref[...], NT).astype(BF).astype(F32)
                for n in range(2):
                    at, up = W * n, gu_ref[n, rows, L:]
                    silu, dg, du = back(gu_ref[n, rows, :L], up, dd[:, L * n : L * n + L])
                    dgu_ref[rows, at : at + L] = dg
                    dgu_ref[rows, at + L : at + W] = du
                    weights[m // D, m % D : m % D + W, L * n : L * n + L] = (silu * up).astype(BF)
            low, high = (dotg(weights[i, :, :W], resident[D * i : D * i + D, :], TN) for i in range(2))
            out_ref[...] = (low + high).astype(BF)

        tiles = pl.BlockSpec((2, T, W), lambda j: (j, 0, 0))
        pipeline(body, (STEPS,), [block(W, D, row), tiles], [block(T, M, col), block(W, D, row)], hooks, full[2], gu0, dgu0, term_d[0])
        send_term(u)

    for u in (0, 1, 4, 5):
        mix_start(u)
    barrier((nx, ny, peer))
    mix_wait(0)
    start_first(0)
    start_rest(0)
    mix_wait(1)
    start_first(1)
    mix_wait(4)
    mix_wait(5)
    pipeline(norm_body, (T // W,), [block(W, D, row)], [block(W, D, row), block(D, W, col)], None, x, a0, a0t)
    in_a = load(a0, resident, 0)
    in_a.start()
    pass_on(0)
    pass_on_last(0)
    in_a.wait()
    arrived(0)
    gate_up0(0, {6: lambda: pass_on(1)})
    pass_on_last(1)
    arrived(1)
    gate_up0(1, {6: lambda: pass_on(2)})
    in_dy = load(dy, resident, 0)
    in_dy.start()
    pass_on_last(2)
    arrived(2)
    pl.run_scoped(down_op, VMEM((FF, D), BF), pltpu.SemaphoreType.DMA)
    in_at = load(a1t, resident_t, 1)
    in_at.start()
    in_dy.wait()
    pass_on_last(3)
    arrived(3)
    pipeline(dact_body, (STEPS,), [block(W, D, row)], [block(T, W, col)], {6: lambda: pass_on(4)}, full[3], dact1)
    in_a = load(a1, resident, 0)
    in_a.start()
    in_dy = [load(dy.at[pl.ds(D * i, D), :], weights.at[i, :, pl.ds(0, D)], 2 + i) for i in range(2)]
    for c in in_dy:
        c.start()
    pass_on_last(4)
    in_at.wait()
    in_a.wait()
    for c in in_dy:
        c.wait()
    arrived(4)
    gate_up1(0, {6: lambda: pass_on(5)})
    pass_on_last(5)
    arrived(5)
    gate_up1(1, None)
    send_term(3)
    in_w = [load(full[4 + i], weights.at[i], 2 + i) for i in range(2)]
    for c in in_w:
        c.start()
    for u in range(6):
        for k in range(11):
            hop(u, k).wait_send()
    grad_gu(1, 4, 5, dgu1, {2: fetch1(3), 3: pass1(3), 7: (fetch2(3),), 8: pass2(3), 10: fetch1(4)})
    in_at = load(a0t, resident_t, 1)
    in_at.start()
    for c in in_w:
        c.wait()
    grad_in(dgu1, h1, dy, dh1, True, {0: pass1(4), 1: fetch3(3), 2: pass3(3), 3: fetch1(5), 4: together(pass1(5), fetch2(4)), 5: pass2(4)})
    act_back(2, {2: fetch2(5), 3: pass2(5), 4: fetch3(4), 5: pass3(4), 8: fetch3(5), 9: pass3(5)})
    in_w = [load(full[i], weights.at[i], 2 + i) for i in range(2)]
    for c in in_w:
        c.start()
    in_at.wait()
    grad_gu(0, 0, 1, dgu0, {2: fetch1(2), 3: pass1(2), 6: fetch2(2), 7: (pass2(2),), 10: fetch1(0)})
    for c in in_w:
        c.wait()
    grad_in(dgu0, x, dh1, dx, False, {0: pass1(0), 1: fetch3(2), 2: together(pass3(2), fetch1(1)), 3: together(pass1(1), fetch2(0)), 4: pass2(0), 6: fetch2(1)})
    pass2(1)()
    fetch3(0)()
    pass3(0)()
    fetch3(1)()
    pass3(1)()
    for u in (1, 2):
        for k in range(4, 8):
            copy(u, k).wait_send()
    for u in range(6):
        for k in range(4):
            copy(u, k).wait_send()


def hand_on_kernel(*refs):
    sources, targets, buffers, sems = refs[:4], refs[4:8], refs[8:12], refs[12]
    arrays = range(4)
    ins = [pltpu.make_async_copy(sources[i], buffers[i], sems.at[i]) for i in arrays]
    outs = [pltpu.make_async_copy(buffers[i], targets[i], sems.at[4 + i]) for i in arrays]
    for c in ins:
        c.start()
    for c, o in zip(ins, outs):
        c.wait()
        o.start()
    for o in outs:
        o.wait()


def solution(mesh):
    any_ = pl.BlockSpec(memory_space=ANY)
    dma = pltpu.SemaphoreType.DMA

    def s(*shape, dtype=BF):
        return jax.ShapeDtypeStruct(shape, dtype)

    outs = [s(2, GROWS, FF), s(2, GROWS, FF), s(2, DROWS, D), s(T, D)]
    outs += [s(*full_shape(u)) for u in range(6)]
    outs += [s(D, 2 * FF)] * 2 + [s(FF, D)] * 2
    outs += [s(4 * rows_of(u), full_shape(u)[1]) for u in range(6)]
    outs += [s(T, D), s(D, T), s(T, D), s(T, D), s(D, T), s(T, FF), s(2 * STEPS, T, W, dtype=F32), s(T, 2 * FF), s(T, FF), s(T, D), s(T, 2 * FF)]
    scratch = [VMEM((2, D, FF), BF), VMEM((T, D), BF), VMEM((D, T), BF)]
    scratch += [VMEM((4, r, FF), BF) for r in (GROWS // 2, GROWS // 2, GROWS, GROWS)]
    scratch += [VMEM((2, r, D), BF) for r in (DROWS // 2, DROWS // 2, DROWS, DROWS)]
    scratch += [VMEM((3, GROWS, FF), BF), VMEM((3, DROWS, D), BF), VMEM((4, GROWS, FF), BF), VMEM((4, DROWS, D), BF)]
    scratch += [dma((6, 11)), dma((6, 11)), dma((6, 8)), dma((6, 8)), dma((6,)), dma((6,)), dma((4,)), dma((4,)), dma((2,))]
    step = pl.pallas_call(
        kernel,
        out_shape=outs,
        in_specs=[any_] * 4 + [pl.BlockSpec(memory_space=VMEM)],
        out_specs=[any_] * len(outs),
        scratch_shapes=scratch,
        compiler_params=pltpu.CompilerParams(collective_id=0, has_side_effects=True, vmem_limit_bytes=63 << 20),
        name="step",
    )

    hand_on = pl.pallas_call(
        hand_on_kernel,
        out_shape=outs[:4],
        in_specs=[any_] * 4,
        out_specs=[any_] * 4,
        scratch_shapes=[VMEM(o.shape, BF) for o in outs[:4]] + [dma((8,))],
        name="hand_on",
    )

    def body(x, dy, wg, wu, wd):
        by_g, by_u, by_d, dx = hand_on(*step(x[0], dy[0], wg, wu, wd)[:4])
        return dx[None], by_g, by_u, by_d

    seq, rows = P(("rep", "dp"), None, None), P(None, "dp", None)
    out = P("rep", "dp", None)
    return jax.shard_map(body, mesh=mesh, in_specs=(seq, seq, rows, rows, rows), out_specs=(seq, out, out, out), check_vma=False)
```

```python
import jax
import jax.numpy as jnp
from jax import lax
from jax.experimental import pallas as pl
from jax.experimental.pallas import tpu as pltpu
from jax.sharding import PartitionSpec as P

BF, F32 = jnp.bfloat16, jnp.float32
T, D, FF = 2048, 1024, 2816
H = FF // 2
GROWS, DROWS = D // 8, FF // 8
UNITS = ((0, 0), (0, 1), (0, 2), (1, 2), (1, 0), (1, 1))
NT = (((1,), (1,)), ((), ()))
TN = (((0,), (0,)), ((), ()))
VMEM = pltpu.VMEM
ANY = pl.ANY
L, W, M = 128, 256, 512
STEPS = FF // W


def rows_of(u):
    return DROWS if UNITS[u][1] == 2 else GROWS


def full_shape(u):
    return (FF, D) if UNITS[u][1] == 2 else (D, FF)


def sigmoid(z):
    return 0.5 * jnp.tanh(0.5 * z) + 0.5


def dot(a, b):
    return jnp.dot(a, b, preferred_element_type=F32)


def dotg(a, b, dims):
    return lax.dot_general(a, b, dims, preferred_element_type=F32)


def places():
    me = lax.axis_index("dp")
    ix, iy, ic = me // 4, (me // 2) % 2, me % 2
    flip = lambda a, b, c: (ix + a - 2 * a * ix) * 4 + (iy + b - 2 * b * iy) * 2 + (ic + c - 2 * c * ic)
    return me, flip


def barrier(peers):
    sem = pltpu.get_barrier_semaphore()
    for p in peers:
        pl.semaphore_signal(sem, inc=1, device_id={"dp": p}, device_id_type=pl.DeviceIdType.MESH)
    pl.semaphore_wait(sem, len(peers))


def remote(src, dst, send, recv, to):
    return pltpu.make_async_remote_copy(src_ref=src, dst_ref=dst, send_sem=send, recv_sem=recv, device_id={"dp": to}, device_id_type=pl.DeviceIdType.MESH)


def block(rows, cols, index):
    return pl.BlockSpec((rows, cols), index)


def deep(rows, cols, index):
    return pl.BlockSpec((rows, cols), index, pipeline_mode=pl.Buffered(3))


def row(i):
    return i, 0


def col(j):
    return 0, j


def pipeline(body, grid, ins, outs, hooks, *arrays):
    def run(*refs):
        step = pl.program_id(0)
        if len(grid) == 2:
            step = step * grid[1] + pl.program_id(1)
        for at, work in (hooks or {}).items():
            pl.when(step == at)(work)
        body(*refs)

    pltpu.emit_pipeline(run, grid=grid, in_specs=ins, out_specs=outs)(*arrays)


def inverse_rms(wide):
    return lax.rsqrt(jnp.mean(wide * wide, -1, keepdims=True) + 1e-6)


def kernel(x, dy, wg, wu, wd, *refs):
    (by_g, by_u, by_d, dx), refs = refs[:4], refs[4:]
    full, term_gu, term_d, from_peer, refs = refs[:6], refs[6:8], refs[8:10], refs[10:16], refs[16:]
    a0, a0t, h1, a1, a1t, act0, gu0, dgu1, dact1, dh1, dgu0, refs = *refs[:11], refs[11:]
    weights, resident, resident_t, *landings, gsend, dsend, gload, dload, gsem, gsem2, send, recv, local, mix, extra, lsem, osem = refs
    me, flip = places()
    nx, ny, peer, nxy = flip(1, 0, 0), flip(0, 1, 0), flip(0, 0, 1), flip(1, 1, 0)
    shards = [wd.at[n] if half == 2 else gload.at[2 * n + half] for n, half in UNITS]

    def load(src, dst, n):
        return pltpu.make_async_copy(src, dst, extra.at[n])

    def kind(u):
        return UNITS[u][1] == 2


    def part(u, b, half=None):
        r = rows_of(u)
        if half is None:
            return full[u].at[pl.ds(b * r, r), :]
        return full[u].at[pl.ds(b * r + half * (r // 2), r // 2), :]

    def piece(u):
        return 96 if kind(u) else 32

    def hop(u, k):
        r, p = rows_of(u), piece(u)
        low, high = pl.ds(0, p), pl.ds(p, r - p)
        mine = part(u, me)
        src, dst, to = (
            (shards[u].at[high, :], mine.at[high, :], nx),
            (shards[u].at[high, :], mine.at[high, :], ny),
            (shards[u], mine, peer),
            (part(u, nx, 0), part(u, nx, 0), ny),
            (part(u, ny, 1), part(u, ny, 1), nx),
            (part(u, nx), part(u, nx), peer),
            (part(u, ny), part(u, ny), peer),
            (part(u, nxy, 0), part(u, nxy, 0), peer),
            (part(u, nxy, 1), part(u, nxy, 1), peer),
            (shards[u].at[low, :], mine.at[low, :], nx),
            (shards[u].at[low, :], mine.at[low, :], ny),
        )[k]
        return remote(src, dst, gsem.at[u, k], gsem2.at[u, k], to)

    def own_copy(u):
        return pltpu.make_async_copy(shards[u], part(u, me), local.at[u])

    def start_first(u):
        hop(u, 9).start()
        hop(u, 10).start()

    def start_rest(u):
        for k in range(3):
            hop(u, k).start()
        own_copy(u).start()

    def pass_on(u):
        for k in (0, 1):
            hop(u, k + 9).wait_recv()
            hop(u, k).wait_recv()
            hop(u, k + 3).start()
            hop(u, k + 5).start()
        if u < 5:
            start_rest(u + 1)
        if u < 4:
            start_first(u + 2)

    def pass_on_last(u):
        for k in (3, 4):
            hop(u, k).wait_recv()
            hop(u, k + 4).start()

    def arrived(u):
        own_copy(u).wait()
        for k in (2, 5, 6, 7, 8):
            hop(u, k).wait_recv()

    def mix_start(u):
        n, half = UNITS[u]
        for j in range(STEPS):
            cols = pl.ds(half * H + L * j, L)
            for i, w in enumerate((wg, wu)):
                pltpu.make_async_copy(w.at[n, :, cols], shards[u].at[:, pl.ds(W * j + L * i, L)], mix.at[u]).start()

    def mix_wait(u):
        pltpu.make_async_copy(shards[u], shards[u], mix.at[u]).wait()

    where = (me, nx, ny, nxy)

    slot = (0, 1, 0, 1, 2, 3)
    before = {5: 4, 0: 5, 1: 0, 2: 3}

    def landing(u):
        return tuple(t.at[slot[u]] for t in landings[4 * kind(u) : 4 * kind(u) + 4])

    def sending(u):
        return dsend if kind(u) else gsend

    def loading(u):
        return dload if kind(u) else gload

    def term(u, b):
        n, half = UNITS[u]
        rows = pl.ds(b * rows_of(u), rows_of(u))
        return term_d[n].at[rows, :] if half == 2 else term_gu[n].at[rows, pl.ds(half * FF, FF)]

    def copy(u, k):
        r = rows_of(u)
        if k < 4:
            b = where[k]
            other = b + 1 - 2 * (b % 2)
            return remote(term(u, other), from_peer[u].at[pl.ds((b // 2) * r, r), :], send.at[u, k], recv.at[u, k], peer)
        s, (l1x, l1y, l2x, l2y) = sending(u), landing(u)
        half = r // 2
        src, dst, to = (
            (s.at[0, pl.ds(0, half), :], l1x, nx),
            (s.at[0, pl.ds(half, half), :], l1y, ny),
            (s.at[1], l2x, nx),
            (s.at[2], l2y, ny),
        )[k - 4]
        return remote(src, dst, send.at[u, k], recv.at[u, k], to)

    def send_term(u):
        for k in (3, 1, 2, 0):
            copy(u, k).start()

    def pairs(u, qs):
        r, v = rows_of(u), loading(u)
        for n, q in enumerate(qs):
            b = where[q]
            yield pltpu.make_async_copy(term(u, b), v.at[n], lsem.at[2 * n])
            yield pltpu.make_async_copy(from_peer[u].at[pl.ds((b // 2) * r, r), :], v.at[n + 2], lsem.at[2 * n + 1])

    def fetch(u, *qs):
        for q in qs:
            copy(u, q).wait_recv()
        for c in pairs(u, qs):
            c.start()

    def fetched(u, *qs):
        for c in pairs(u, qs):
            c.wait()

    def chunks(count, body):
        def step(i, _):
            body(pl.multiple_of(i * 16, 16))
            return 0

        lax.fori_loop(0, count // 16, step, 0)

    def both(v, n, rows):
        return v[n, rows, :].astype(F32) + v[n + 2, rows, :].astype(F32)

    def sent_before(u, *ks):
        if u in before:
            for k in ks:
                copy(before[u], k).wait_send()

    def fetch1(u):
        return lambda: fetch(u, 3)

    def fetch2(u):
        return lambda: fetch(u, 1, 2)

    def fetch3(u):
        return lambda: fetch(u, 0)

    def pass1(u):
        def work():
            fetched(u, 3)
            v, s = loading(u), sending(u)
            sent_before(u, 4, 5)

            def body(at):
                rows = pl.ds(at, 16)
                s[0, rows, :] = both(v, 0, rows).astype(BF)

            chunks(rows_of(u), body)
            copy(u, 4).start()
            copy(u, 5).start()

        return work

    def pass2(u):
        def work():
            fetched(u, 1, 2)
            v, s = loading(u), sending(u)
            l1x, l1y, _, _ = landing(u)
            sent_before(u, 6, 7)
            half = rows_of(u) // 2
            copy(u, 4).wait_recv()
            copy(u, 5).wait_recv()

            def body(at):
                low, high = pl.ds(at, 16), pl.ds(at + half, 16)
                s[1, low, :] = both(v, 0, low).astype(BF)
                s[1, high, :] = (both(v, 0, high) + l1y[low, :].astype(F32)).astype(BF)
                s[2, low, :] = (both(v, 1, low) + l1x[low, :].astype(F32)).astype(BF)
                s[2, high, :] = both(v, 1, high).astype(BF)

            chunks(half, body)
            copy(u, 6).start()
            copy(u, 7).start()

        return work

    def pass3(u):
        def work():
            fetched(u, 0)
            v = loading(u)
            _, _, l2x, l2y = landing(u)
            copy(u, 6).wait_recv()
            copy(u, 7).wait_recv()
            n, half = UNITS[u]

            def body(at):
                rows = pl.ds(at, 16)
                total = (both(v, 0, rows) + l2x[rows, :].astype(F32) + l2y[rows, :].astype(F32)).astype(BF)
                if kind(u):
                    v[1, rows, :] = total
                    return
                for j in range(STEPS):
                    for i in range(2):
                        v[1, rows, H * i + L * j : H * i + L * j + L] = total[:, W * j + L * i : W * j + L * i + L]

            chunks(rows_of(u), body)
            if kind(u):
                copies = [pltpu.make_async_copy(v.at[1], by_d.at[n], osem.at[0])]
            else:
                cols = pl.ds(half * H, H)
                copies = [pltpu.make_async_copy(v.at[1, :, pl.ds(H * i, H)], t.at[n, :, cols], osem.at[i]) for i, t in enumerate((by_g, by_u))]
            for c in copies:
                c.start()
            for c in copies:
                c.wait()

        return work

    def together(*works):
        def work():
            for w in works:
                w()

        return work


    def norm_into(wide, a_ref, at_ref):
        a = (wide * inverse_rms(wide)).astype(BF)
        a_ref[...] = a
        at_ref[...] = a.T

    def norm_body(x_ref, a_ref, at_ref):
        norm_into(x_ref[...].astype(F32), a_ref, at_ref)

    def gate_up0(half, hooks):
        def body(w_ref, gu_ref, act_ref):
            for m in range(0, T, M):
                s = dot(resident[m : m + M, :], w_ref[...])
                gu_ref[m : m + M, :] = s
                g, up = s[:, :L], s[:, L:]
                act_ref[m : m + M, :] = (g * sigmoid(g) * up).astype(BF)

        cols = lambda j: (0, j + STEPS * half)
        tiles = pl.BlockSpec((None, T, W), lambda j: (j + STEPS * half, 0, 0))
        pipeline(body, (STEPS,), [block(D, W, col)], [tiles, block(T, L, cols)], hooks, full[half], gu0, act0)

    def down_op(down, sem):
        in_down = pltpu.make_async_copy(full[2], down, sem)
        in_down.start()
        in_down.wait()

        def body(act_ref, x_ref, h_ref, a_ref, at_ref):
            h = x_ref[...] + dot(act_ref[...], down[...]).astype(BF)
            h_ref[...] = h
            norm_into(h.astype(F32), a_ref, at_ref)

        outs = [block(M, D, row), block(M, D, row), block(D, M, col)]
        pipeline(body, (T // M,), [block(M, FF, row), block(M, D, row)], outs, {2: lambda: pass_on(3)}, act0, x, h1, a1, a1t)

    def dact_body(w_ref, out_ref):
        for m in range(0, T, M):
            out_ref[m : m + M, :] = dotg(resident[m : m + M, :], w_ref[...], NT).astype(BF)

    def back(g, up, d):
        sg = sigmoid(g)
        silu = g * sg
        return silu, (d * up * (sg + silu * (1.0 - sg))).astype(BF), (d * silu).astype(BF)

    def gate_up1(half, hooks):
        def body(w_ref, dact_ref, dgu_ref, out_ref):
            for m in range(0, T, M):
                rows = slice(m, m + M)
                s = dot(resident[rows, :], w_ref[...])
                up = s[:, L:]
                silu, dg, du = back(s[:, :L], up, dact_ref[rows, :].astype(F32))
                weights[m // D, m % D : m % D + M, D : D + L] = (silu * up).astype(BF)
                dgu_ref[rows, :L] = dg
                dgu_ref[rows, L:] = du
            low, high = (dotg(weights[i, :, D : D + L], weights[i, :, :D], TN) for i in range(2))
            out_ref[...] = (low + high).astype(BF)

        cols = lambda j: (0, j + STEPS * half)
        ins, outs = [block(D, W, col), block(T, L, cols)], [block(T, W, cols), block(L, D, lambda j: (j + STEPS * half, 0))]
        pipeline(body, (STEPS,), ins, outs, hooks, full[4 + half], dact1, dgu1, term_d[1])

    def grad_gu(n, first, second, dgu, hooks):
        def body(d_ref, out_ref):
            for m in range(0, D, M):
                out_ref[m : m + M, :] = dot(resident_t[m : m + M, :], d_ref[...]).astype(BF)

        early = {7: together(*hooks.pop(7, ()), lambda: send_term(first))}
        pipeline(body, (STEPS,), [deep(T, M, col)], [block(D, M, col)], hooks | early, dgu, term_gu[n])
        send_term(second)

    def grad_in(dgu, h, dh, out, keep, hooks):
        def body(d_ref, h_ref, dh_ref, out_ref):
            da = dotg(d_ref[:, :FF], weights[0], NT) + dotg(d_ref[:, FF:], weights[1], NT)
            d = da.astype(BF).astype(F32)
            wide = h_ref[...].astype(F32)
            scale = inverse_rms(wide)
            by_h = d * scale - wide * (scale * scale * scale * jnp.mean(d * wide, -1, keepdims=True))
            total = dh_ref[...] + by_h.astype(BF)
            out_ref[...] = total
            if keep:
                resident[pl.ds(pl.multiple_of(pl.program_id(0) * W, W), W), :] = total

        pipeline(body, (T // W,), [block(W, 2 * FF, row)] + [block(W, D, row)] * 2, [block(W, D, row)], hooks, dgu, h, dh, out)

    def act_back(u, hooks):
        def body(w_ref, gu_ref, dgu_ref, out_ref):
            for m in range(0, T, W):
                rows = slice(m, m + W)
                dd = dotg(resident[rows, :], w_ref[...], NT).astype(BF).astype(F32)
                for n in range(2):
                    at, up = W * n, gu_ref[n, rows, L:]
                    silu, dg, du = back(gu_ref[n, rows, :L], up, dd[:, L * n : L * n + L])
                    dgu_ref[rows, at : at + L] = dg
                    dgu_ref[rows, at + L : at + W] = du
                    weights[m // D, m % D : m % D + W, L * n : L * n + L] = (silu * up).astype(BF)
            low, high = (dotg(weights[i, :, :W], resident[D * i : D * i + D, :], TN) for i in range(2))
            out_ref[...] = (low + high).astype(BF)

        tiles = pl.BlockSpec((2, T, W), lambda j: (j, 0, 0))
        pipeline(body, (STEPS,), [block(W, D, row), tiles], [block(T, M, col), block(W, D, row)], hooks, full[2], gu0, dgu0, term_d[0])
        send_term(u)

    for u in (0, 1, 4, 5):
        mix_start(u)
    barrier((nx, ny, peer))
    mix_wait(0)
    start_first(0)
    start_rest(0)
    mix_wait(1)
    start_first(1)
    mix_wait(4)
    mix_wait(5)
    pipeline(norm_body, (T // W,), [block(W, D, row)], [block(W, D, row), block(D, W, col)], None, x, a0, a0t)
    in_a = load(a0, resident, 0)
    in_a.start()
    pass_on(0)
    pass_on_last(0)
    in_a.wait()
    arrived(0)
    gate_up0(0, {6: lambda: pass_on(1)})
    pass_on_last(1)
    arrived(1)
    gate_up0(1, {6: lambda: pass_on(2)})
    in_dy = load(dy, resident, 0)
    in_dy.start()
    pass_on_last(2)
    arrived(2)
    pl.run_scoped(down_op, VMEM((FF, D), BF), pltpu.SemaphoreType.DMA)
    in_at = load(a1t, resident_t, 1)
    in_at.start()
    in_dy.wait()
    pass_on_last(3)
    arrived(3)
    pipeline(dact_body, (STEPS,), [block(W, D, row)], [block(T, W, col)], {6: lambda: pass_on(4)}, full[3], dact1)
    in_a = load(a1, resident, 0)
    in_a.start()
    in_dy = [load(dy.at[pl.ds(D * i, D), :], weights.at[i, :, pl.ds(0, D)], 2 + i) for i in range(2)]
    for c in in_dy:
        c.start()
    pass_on_last(4)
    in_at.wait()
    in_a.wait()
    for c in in_dy:
        c.wait()
    arrived(4)
    gate_up1(0, {6: lambda: pass_on(5)})
    pass_on_last(5)
    arrived(5)
    gate_up1(1, None)
    send_term(3)
    in_w = [load(full[4 + i], weights.at[i], 2 + i) for i in range(2)]
    for c in in_w:
        c.start()
    for u in range(6):
        for k in range(11):
            hop(u, k).wait_send()
    grad_gu(1, 4, 5, dgu1, {2: fetch1(3), 3: pass1(3), 7: (fetch2(3),), 8: pass2(3), 10: fetch1(4)})
    in_at = load(a0t, resident_t, 1)
    in_at.start()
    for c in in_w:
        c.wait()
    grad_in(dgu1, h1, dy, dh1, True, {0: pass1(4), 1: fetch3(3), 2: pass3(3), 3: fetch1(5), 4: together(pass1(5), fetch2(4)), 5: pass2(4)})
    act_back(2, {2: fetch2(5), 3: pass2(5), 4: fetch3(4), 5: pass3(4), 8: fetch3(5), 9: pass3(5)})
    in_w = [load(full[i], weights.at[i], 2 + i) for i in range(2)]
    for c in in_w:
        c.start()
    in_at.wait()
    grad_gu(0, 0, 1, dgu0, {2: fetch1(2), 3: pass1(2), 6: fetch2(2), 7: (pass2(2),), 10: fetch1(0)})
    for c in in_w:
        c.wait()
    grad_in(dgu0, x, dh1, dx, False, {0: pass1(0), 1: fetch3(2), 2: together(pass3(2), fetch1(1)), 3: together(pass1(1), fetch2(0)), 4: pass2(0), 6: fetch2(1)})
    pass2(1)()
    fetch3(0)()
    pass3(0)()
    fetch3(1)()
    pass3(1)()
    for u in (1, 2):
        for k in range(4, 8):
            copy(u, k).wait_send()
    for u in range(6):
        for k in range(4):
            copy(u, k).wait_send()


def hand_on_kernel(*refs):
    sources, targets, buffers, sems = refs[:4], refs[4:8], refs[8:12], refs[12]
    pieces = [(3, pl.ds(M * i, M)) for i in range(T // M)] + [(i, pl.ds(0, 2)) for i in range(3)]
    ins = [pltpu.make_async_copy(sources[i].at[p], buffers[i].at[p], sems.at[0, n]) for n, (i, p) in enumerate(pieces)]
    outs = [pltpu.make_async_copy(buffers[i].at[p], targets[i].at[p], sems.at[1, n]) for n, (i, p) in enumerate(pieces)]
    for c in ins:
        c.start()
    for c, o in zip(ins, outs):
        c.wait()
        o.start()
    for o in outs:
        o.wait()


def solution(mesh):
    any_ = pl.BlockSpec(memory_space=ANY)
    dma = pltpu.SemaphoreType.DMA

    def s(*shape, dtype=BF):
        return jax.ShapeDtypeStruct(shape, dtype)

    outs = [s(2, GROWS, FF), s(2, GROWS, FF), s(2, DROWS, D), s(T, D)]
    outs += [s(*full_shape(u)) for u in range(6)]
    outs += [s(D, 2 * FF)] * 2 + [s(FF, D)] * 2
    outs += [s(4 * rows_of(u), full_shape(u)[1]) for u in range(6)]
    outs += [s(T, D), s(D, T), s(T, D), s(T, D), s(D, T), s(T, FF), s(2 * STEPS, T, W, dtype=F32), s(T, 2 * FF), s(T, FF), s(T, D), s(T, 2 * FF)]
    scratch = [VMEM((2, D, FF), BF), VMEM((T, D), BF), VMEM((D, T), BF)]
    scratch += [VMEM((4, r, FF), BF) for r in (GROWS // 2, GROWS // 2, GROWS, GROWS)]
    scratch += [VMEM((2, r, D), BF) for r in (DROWS // 2, DROWS // 2, DROWS, DROWS)]
    scratch += [VMEM((3, GROWS, FF), BF), VMEM((3, DROWS, D), BF), VMEM((4, GROWS, FF), BF), VMEM((4, DROWS, D), BF)]
    scratch += [dma((6, 11)), dma((6, 11)), dma((6, 8)), dma((6, 8)), dma((6,)), dma((6,)), dma((4,)), dma((4,)), dma((2,))]
    step = pl.pallas_call(
        kernel,
        out_shape=outs,
        in_specs=[any_] * 4 + [pl.BlockSpec(memory_space=VMEM)],
        out_specs=[any_] * len(outs),
        scratch_shapes=scratch,
        compiler_params=pltpu.CompilerParams(collective_id=0, has_side_effects=True, vmem_limit_bytes=63 << 20),
        name="step",
    )

    hand_on = pl.pallas_call(
        hand_on_kernel,
        out_shape=outs[:4],
        in_specs=[any_] * 4,
        out_specs=[any_] * 4,
        scratch_shapes=[VMEM(o.shape, BF) for o in outs[:4]] + [dma((2, 7))],
        name="hand_on",
    )

    def body(x, dy, wg, wu, wd):
        by_g, by_u, by_d, dx = hand_on(*step(x[0], dy[0], wg, wu, wd)[:4])
        return dx[None], by_g, by_u, by_d

    seq, rows = P(("rep", "dp"), None, None), P(None, "dp", None)
    out = P("rep", "dp", None)
    return jax.shard_map(body, mesh=mesh, in_specs=(seq, seq, rows, rows, rows), out_specs=(seq, out, out, out), check_vma=False)
```
